256 devices in a mesh: rep: 2 (over core), dp: 128 (over x, y, z).
Axes of the slice: x: 4, y: 4, z: 8, core: 2. Of those that a mesh axis runs over, the one named last changes fastest.
Arguments:
- x: bfloat16 [256, 2048, 512], P(('rep', 'dp')), parts along dimension 0
- dy: bfloat16 [256, 2048, 512], P(('rep', 'dp')), parts along dimension 0
- w_gate: bfloat16 [2, 512, 3072], replicated
- w_up: bfloat16 [2, 512, 3072], replicated
- w_down: bfloat16 [2, 3072, 512], replicated
- m_w_gate: float32 [2, 512, 3072], P(None, 'dp')
- m_w_up: float32 [2, 512, 3072], P(None, 'dp')
- m_w_down: float32 [2, 3072, 512], P(None, 'dp')
- v_w_gate: float32 [2, 512, 3072], P(None, 'dp')
- v_w_up: float32 [2, 512, 3072], P(None, 'dp')
- v_w_down: float32 [2, 3072, 512], P(None, 'dp')
Outputs:
- output 1: bfloat16 [4, 512, 3072], P('rep'), parts along dimension 0
- output 2: bfloat16 [4, 512, 3072], P('rep'), parts along dimension 0
- output 3: bfloat16 [4, 3072, 512], P('rep'), parts along dimension 0
- output 4: float32 [4, 512, 3072], P('rep', 'dp'), parts along dimension 0
- output 5: float32 [4, 512, 3072], P('rep', 'dp'), parts along dimension 0
- output 6: float32 [4, 3072, 512], P('rep', 'dp'), parts along dimension 0
- output 7: float32 [4, 512, 3072], P('rep', 'dp'), parts along dimension 0
- output 8: float32 [4, 512, 3072], P('rep', 'dp'), parts along dimension 0
- output 9: float32 [4, 3072, 512], P('rep', 'dp'), parts along dimension 0
There are 2 independent parts. The reference program is written for one: setup_inputs(seed, part) draws one part's arguments, and reference() takes and returns one part's arrays. A program takes and returns all parts, laid end to end along the dimension named above; an argument that names none is the same for every part.
All inputs are finite; a program needn't handle non-finite values.
Results may differ from the reference program's by a relative error of at most 0.022.
Values are sent between devices in bfloat16 or wider.
A program may use at most 768 MiB of HBM per device.

```python
import jax
import jax.numpy as jnp
from jax import lax

SEQUENCES = 128
TOKENS = 2048
D = 512
FF = 3072
LAYERS = 2
NAMES = ("w_gate", "w_up", "w_down")
SHAPES = {"w_gate": (LAYERS, D, FF), "w_up": (LAYERS, D, FF), "w_down": (LAYERS, FF, D)}


def bump(key, n, height):
    away = (jnp.arange(n, dtype=jnp.int32) - jax.random.randint(key, (), 0, n, jnp.int32)) % n
    return jnp.where(away < n // 8, height, 1.0)


def together(key, own, strength):
    shared = jax.random.normal(key, own.shape[1:], jnp.float32)
    return (own + strength * shared) * lax.rsqrt(1 + strength * strength)


def setup_inputs(seed: int = 0, part: int = 0) -> dict:
    kx, kdy, ka, kb, kz, kf, kh, kl, *keys = jax.random.split(jax.random.key(seed), 8 + 3 * len(NAMES))
    kx, kdy, ka, kb = (jax.random.fold_in(k, part) for k in (kx, kdy, ka, kb))
    kw, km, kv = (keys[i::3] for i in range(3))
    shape = (SEQUENCES, TOKENS, D)
    much_x, much_dy = jax.random.uniform(kz, (2,), jnp.float32, 0.0, 1.0)
    loud = 2.0 ** jax.random.uniform(jax.random.fold_in(kz, 1), (), jnp.float32, -1.0, 2.0)
    layers = 2.0 ** jax.random.uniform(kl, (LAYERS, 1, 1), jnp.float32, -1.0, 1.0)
    x = together(ka, jax.random.normal(kx, shape, jnp.float32), much_x) * bump(kf, D, 4.0)
    dy = together(kb, jax.random.normal(kdy, shape, jnp.float32), much_dy)
    drawn = {"x": x.astype(jnp.bfloat16), "dy": (loud * dy * (SEQUENCES * TOKENS) ** -0.5).astype(jnp.bfloat16)}
    for key, name in zip(kw, NAMES, strict=True):
        w = jax.random.normal(key, SHAPES[name], jnp.float32) * SHAPES[name][1] ** -0.5
        drawn[name] = (w * {"w_gate": 1.0, "w_up": bump(kh, FF, 4.0), "w_down": layers}[name]).astype(jnp.bfloat16)
    for key, name in zip(km, NAMES, strict=True):
        drawn[f"m_{name}"] = 0.1 * jax.random.normal(key, SHAPES[name], jnp.float32)
    for key, name in zip(kv, NAMES, strict=True):
        drawn[f"v_{name}"] = loud * loud * jax.random.uniform(key, SHAPES[name], jnp.float32, 0.05, 0.15)
    return drawn


def matmul(a, w):
    return jnp.dot(a, w, preferred_element_type=jnp.float32).astype(jnp.bfloat16)


def normed(h):
    wide = h.astype(jnp.float32)
    scale = lax.rsqrt(jnp.mean(wide**2, -1, keepdims=True) + 1e-6)
    return (wide * scale).astype(jnp.bfloat16)


def layer(h, w):
    a = normed(h)
    gate = jnp.dot(a, w["w_gate"], preferred_element_type=jnp.float32)
    up = jnp.dot(a, w["w_up"], preferred_element_type=jnp.float32)
    return h + matmul((jax.nn.silu(gate) * up).astype(jnp.bfloat16), w["w_down"])


def adamw(w, m, v, g):
    m = 0.9 * m + 0.1 * g
    v = 0.95 * v + 0.05 * g * g
    step = m * lax.rsqrt(v + 1e-8) + 0.1 * w
    return (w - 0.02 * step).astype(jnp.bfloat16), m, v


def stack(weights, h):
    return lax.scan(lambda h, w: (layer(h, w), None), h, weights)[0]


def reference(x, dy, w_gate, w_up, w_down, m_w_gate, m_w_up, m_w_down, v_w_gate, v_w_up, v_w_down):
    weights = dict(zip(NAMES, (w_gate, w_up, w_down), strict=True))

    def take(so_far, sequence):
        h, by_y = sequence
        _, back = jax.vjp(lambda w: stack(w, h), weights)
        return jax.tree.map(lambda total, term: total + term.astype(jnp.float32), so_far, back(by_y)[0]), None

    none_yet = {name: jnp.zeros(w.shape, jnp.float32) for name, w in weights.items()}
    by_weights, _ = lax.scan(take, none_yet, (x, dy))
    gradients = [by_weights[name].astype(jnp.bfloat16).astype(jnp.float32) for name in NAMES]
    new = [
        adamw(w.astype(jnp.float32), m, v, g)
        for w, m, v, g in zip((w_gate, w_up, w_down), (m_w_gate, m_w_up, m_w_down), (v_w_gate, v_w_up, v_w_down), gradients, strict=True)
    ]
    return tuple(one[which] for which in range(3) for one in new)
```

```python
import jax
import jax.numpy as jnp
from jax import lax
from jax.experimental import pallas as pl
from jax.experimental.pallas import tpu as pltpu
from jax.sharding import PartitionSpec as P

MESH = pl.DeviceIdType.MESH
F32, BF16 = jnp.float32, jnp.bfloat16
TOK, D, FF = 2048, 512, 3072
CW = 768
HW = CW // 2
HF = FF // 2
HD = D // 2
LN = 128
CHUNKS = FF // CW
LAST = 2 * CHUNKS
PAIR = (0, 1)
FOUR = range(4)
EIGHT = range(8)
T = 512
SUB = 256


def f32(v):
    return v.astype(F32)


def b16(v):
    return v.astype(BF16)


def dot(a, b):
    return jnp.dot(a, b, preferred_element_type=F32)


def dot_t(a, b):
    return lax.dot_general(a, b, (((1,), (1,)), ((), ())), preferred_element_type=F32)


def rows_of(t, n):
    return pl.ds(pl.multiple_of(t * n, n), n)


def part(i, n):
    return pl.ds(i * n, n)


def flip(p):
    return p + 1 - 2 * lax.rem(p, 2)


def mirror(p):
    return 3 - p


def partners(p, half):
    return (mirror(p), flip(p)) if half else (flip(p), mirror(p))


def passed(p, half):
    first, _ = partners(p, half)
    return first, partners(first, half)[1]


def kept(p, half):
    return p, partners(p, half)[1]


def layer_of(c):
    return jnp.where(c < CHUNKS, 1, 0)


def go(copies):
    for c in copies:
        c.start()


def arrive(copies):
    for c in copies:
        c.wait_recv()


def leave(copies):
    for c in copies:
        c.wait_send()


def adamw(w, m, v, g):
    m = 0.9 * m + 0.1 * g
    v = 0.95 * v + 0.05 * g * g
    step = m * lax.rsqrt(v + 1e-8) + 0.1 * w
    return b16(w - 0.02 * step), m, v


COUNTS = dict(c1=8, c2=4, c3=4, c4=4, cf=7, a0=7, a1=4, a2=8, a3=4, a4=8, ring=14, dy1=2, dy2=2, dx=3, ex=3, ey1=2, ey2=4, back=14)
FIRST = {}
SEMS = 0
for _name, _n in COUNTS.items():
    FIRST[_name] = SEMS
    SEMS += 2 * _n


class Step:
    def __init__(self, refs):
        self.__dict__.update(refs)
        d = lax.axis_index("dp")
        self.rep = lax.axis_index("rep")
        self.x, self.y, self.z = d // 32, lax.rem(d // 8, 4), lax.rem(d, 8)


    def at(self, x=None, y=None, z=None):
        x = self.x if x is None else x
        y = self.y if y is None else y
        z = self.z if z is None else z
        return (self.rep, x * 32 + y * 8 + z)

    def up_z(self, i):
        return lax.rem(self.z + i + 16, 8)

    def up_x(self, i):
        return lax.rem(self.x + i + 4, 4)

    def copy(self, sem, src, dst, dev):
        return pltpu.make_async_remote_copy(
            src_ref=src, dst_ref=dst, send_sem=self.ssem.at[sem], recv_sem=self.rsem.at[sem], device_id=dev, device_id_type=MESH
        )

    def copies(self, name, c, moves):
        base = FIRST[name] + lax.rem(c, 2) * COUNTS[name]
        return [self.copy(base + i, *move) for i, move in enumerate(moves)]

    def barrier(self):
        b = pltpu.get_barrier_semaphore()
        to = [self.at(z=self.up_z(i)) for i in range(1, 8)] + [self.at(x=self.up_x(i)) for i in range(1, 4)]
        to += [self.at(y=flip(self.y)), self.at(y=mirror(self.y))]
        for q in to:
            pl.semaphore_signal(b, inc=1, device_id=q, device_id_type=MESH)
        pl.semaphore_wait(b, len(to))


    def outer(self, w):
        return self.y if w else self.x

    def inner(self, w):
        return self.x if w else self.y

    def at_outer(self, w, p):
        return self.at(y=p) if w else self.at(x=p)

    def at_inner(self, w, p):
        return self.at(x=p) if w else self.at(y=p)

    def halves(self):
        return [(w, h) for w in PAIR for h in PAIR]

    def block(self, w, k, b, h):
        cols = part(h, HW)
        return self.ub.at[k, :, b, :, cols] if w else self.gb.at[k, b, :, :, cols]

    def own(self, w, k, b, j, h):
        cols = part(h, HW)
        return f32(self.ub[k, j, b, :, cols] if w else self.gb[k, b, j, :, cols])

    def c1(self, c):
        k, out = lax.rem(c, 2), []
        for w, h in self.halves():
            first, _ = partners(self.outer(w), h)
            for i, b in enumerate(passed(self.outer(w), h)):
                out.append((self.block(w, k, b, h), self.r1.at[w, k, h, i], self.at_outer(w, first)))
        return self.copies("c1", c, out)

    def c2(self, c):
        k = lax.rem(c, 2)
        return self.copies("c2", c, [(self.s2.at[w, h], self.r2.at[w, k, h], self.at_outer(w, partners(self.outer(w), h)[1])) for w, h in self.halves()])

    def c3(self, c):
        k = lax.rem(c, 2)
        return self.copies("c3", c, [(self.s3.at[w, h], self.r3.at[w, k, h], self.at_inner(w, partners(self.inner(w), h)[0])) for w, h in self.halves()])

    def c4(self, c):
        k = lax.rem(c, 2)
        return self.copies("c4", c, [(self.s4.at[w, h], self.r4.at[w, k, h], self.at_inner(w, partners(self.inner(w), h)[1])) for w, h in self.halves()])

    def cf(self, c):
        zs = [self.up_z(i) for i in range(1, 8)]
        return self.copies("cf", c, [(self.zs.at[z], self.fz.at[i], self.at(z=z)) for i, z in enumerate(zs)])

    def w1(self, c):
        go(self.c1(c))

    def w2(self, c):
        arrive(self.c1(c))
        k = lax.rem(c, 2)
        for w, h in self.halves():
            _, b = partners(self.outer(w), h)
            for j in FOUR:
                self.s2[w, h, j] = b16(self.own(w, k, b, j, h) + f32(self.r1[w, k, h, 1, j]))
        go(self.c2(c))
        leave(self.c1(c))

    def w3(self, c):
        arrive(self.c2(c))
        k = lax.rem(c, 2)
        for w, h in self.halves():
            p, q = self.outer(w), self.inner(w)

            def total(j):
                return self.own(w, k, p, j, h) + f32(self.r1[w, k, h, 0, j]) + f32(self.r2[w, k, h, j])

            for i, j in enumerate(passed(q, h)):
                self.s3[w, h, i] = b16(total(j))
            for i, j in enumerate(kept(q, h)):
                self.keep[w, h, i] = total(j)
        go(self.c3(c))
        leave(self.c2(c))

    def w4(self, c):
        arrive(self.c3(c))
        k = lax.rem(c, 2)
        for w, h in self.halves():
            self.s4[w, h] = b16(self.keep[w, h, 1] + f32(self.r3[w, k, h, 1]))
            self.keep[w, h, 0] += f32(self.r3[w, k, h, 0])
        go(self.c4(c))
        leave(self.c3(c))

    def w5(self, c):
        arrive(self.c4(c))
        k = lax.rem(c, 2)
        for w, h in self.halves():
            v = self.keep[w, h, 0] + f32(self.r4[w, k, h])
            for z in EIGHT:
                self.zf[z, w, h] = v[4 * z : 4 * z + 4]
                self.zs[z, w, h] = b16(v[4 * z : 4 * z + 4])
        self.zo[...] = self.zf[self.z]
        go(self.cf(c))
        leave(self.c4(c))

    def w6(self, c):
        arrive(self.cf(c))
        l, ci = layer_of(c), lax.rem(c, CHUNKS)
        for w, h in self.halves():
            wb, m, v, mo, vo = (getattr(self, s + "gu"[w]) for s in ("w", "m", "v", "mo", "vo"))
            g = self.zo[w, h]
            for i in range(7):
                g = g + f32(self.fz[i, w, h])
            cols = rows_of(2 * ci + h, HW)
            new, mo[l, :, cols], vo[l, :, cols] = adamw(f32(wb[l, :, cols]), m[l, :, cols], v[l, :, cols], f32(b16(g)))
            self.nb[w, h] = new
            self.wz[self.z, w, h] = new
        go(self.a0(c))
        leave(self.cf(c))


    def a0(self, c, get=False):
        zs = [self.up_z(-i if get else i) for i in range(1, 8)]
        return self.copies("a0", c, [(self.nb, self.wz.at[z if get else self.z], self.at(z=z)) for z in zs])

    def cols(self, c, h):
        return rows_of(2 * lax.rem(c, CHUNKS) + h, HW)

    def oblock(self, w, c, b, h):
        l, cols = layer_of(c), self.cols(c, h)
        return self.ou.at[l, b, self.y, :, cols] if w else self.og.at[l, self.x, b, :, cols]

    def obig(self, w, c, b, h):
        l, cols = layer_of(c), self.cols(c, h)
        return self.ou.at[l, :, b, :, cols] if w else self.og.at[l, b, :, :, cols]

    def a1(self, c, get=False):
        out = []
        for w, h in self.halves():
            _, q = partners(self.inner(w), h)
            out.append((self.slab.at[w, h], self.oblock(w, c, q if get else self.inner(w), h), self.at_inner(w, q)))
        return self.copies("a1", c, out)

    def placed(self, c):
        return [pltpu.make_async_copy(self.slab.at[w, h], self.oblock(w, c, self.inner(w), h), self.lsem.at[w, h]) for w, h in self.halves()]

    def a2(self, c, get=False):
        out = []
        for w, h in self.halves():
            first, _ = partners(self.inner(w), h)
            refs = [self.oblock(w, c, b, h) for b in (passed if get else kept)(self.inner(w), h)]
            out += [(ref, ref, self.at_inner(w, first)) for ref in refs]
        return self.copies("a2", c, out)

    def a3(self, c, get=False):
        out = []
        for w, h in self.halves():
            _, q = partners(self.outer(w), h)
            ref = self.obig(w, c, q if get else self.outer(w), h)
            out.append((ref, ref, self.at_outer(w, q)))
        return self.copies("a3", c, out)

    def a4(self, c, get=False):
        out = []
        for w, h in self.halves():
            first, _ = partners(self.outer(w), h)
            refs = [self.obig(w, c, b, h) for b in (passed if get else kept)(self.outer(w), h)]
            out += [(ref, ref, self.at_outer(w, first)) for ref in refs]
        return self.copies("a4", c, out)

    def w7(self, c):
        arrive(self.a0(c, True))
        for w, h in self.halves():
            for z in EIGHT:
                self.slabf[w, h, 4 * z : 4 * z + 4] = f32(self.wz[z, w, h])
            self.slab[w, h] = b16(self.slabf[w, h])
        go(self.a1(c) + self.placed(c))
        leave(self.a0(c))

    def w8(self, c):
        arrive(self.a1(c, True))
        for p in self.placed(c):
            p.wait()
        go(self.a2(c))
        leave(self.a1(c))

    def w9(self, c):
        self.hand_on(self.a2, self.a3, c)

    def w10(self, c):
        self.hand_on(self.a3, self.a4, c)

    def w11(self, c):
        arrive(self.a4(c, True))
        leave(self.a4(c))

    def hand_on(self, before, after, c):
        arrive(before(c, True))
        go(after(c))
        leave(before(c))


    def ring(self, c, s):
        k, out = lax.rem(c, 2), []
        for h in PAIR:
            b, to = (self.up_z(1 + s), self.up_z(-1)) if h else (self.up_z(-1 - s), self.up_z(1))
            src = self.rz.at[k, h, s - 1] if s else self.db.at[k, :, b, :, part(h, HD)]
            out.append((src, self.rz.at[k, h, s], self.at(z=to)))
        return self.ringed("ring", c, s, out)

    def ringed(self, name, c, s, moves):
        base = FIRST[name] + lax.rem(c, 2) * COUNTS[name] + 2 * s
        return [self.copy(base + i, *move) for i, move in enumerate(moves)]

    def d0(self, c):
        go(self.ring(c, 0))

    def turn_ring(self, c, s):
        arrive(self.ring(c, s - 1))
        k = lax.rem(c, 2)
        for h in PAIR:
            b = self.up_z(1 + s) if h else self.up_z(-1 - s)
            for j in FOUR:
                self.rz[k, h, s - 1, j] = b16(f32(self.rz[k, h, s - 1, j]) + f32(self.db[k, j, b, :, part(h, HD)]))
        go(self.ring(c, s))
        leave(self.ring(c, s - 1))

    def dy1(self, c):
        k = lax.rem(c, 2)
        return self.copies("dy1", c, [(self.sdy1.at[h], self.rdy1.at[k, h], self.at(y=partners(self.y, h)[0])) for h in PAIR])

    def dy2(self, c):
        k = lax.rem(c, 2)
        return self.copies("dy2", c, [(self.sdy2.at[h], self.rdy2.at[k, h], self.at(y=partners(self.y, h)[1])) for h in PAIR])

    def d7(self, c):
        arrive(self.ring(c, 6))
        k = lax.rem(c, 2)
        for h in PAIR:

            def total(j):
                return f32(self.rz[k, h, 6, j]) + f32(self.db[k, j, self.z, :, part(h, HD)])

            for i, j in enumerate(passed(self.y, h)):
                self.sdy1[h, i] = b16(total(j))
            for i, j in enumerate(kept(self.y, h)):
                self.kdy[h, i] = total(j)
        go(self.dy1(c))
        leave(self.ring(c, 6))

    def d8(self, c):
        arrive(self.dy1(c))
        k = lax.rem(c, 2)
        for h in PAIR:
            self.sdy2[h] = b16(self.kdy[h, 1] + f32(self.rdy1[k, h, 1]))
            self.kdy[h, 0] += f32(self.rdy1[k, h, 0])
        go(self.dy2(c))
        leave(self.dy1(c))

    def away(self, c):
        return self.up_x(-lax.rem(c, CHUNKS))

    def owner_sem(self, name, c):
        return FIRST[name] + lax.rem(c, 2) * COUNTS[name] - 1

    def dx(self, c):
        i = self.away(c)
        return self.copy(self.owner_sem("dx", c) + i, self.xb, self.fx.at[layer_of(c), i - 1], self.at(x=lax.rem(c, CHUNKS)))

    def dx_in(self, c, i):
        return self.copy(self.owner_sem("dx", c) + i, self.xb, self.fx.at[layer_of(c), i - 1], self.at(x=self.up_x(i)))

    def dblock(self, c, y, z):
        return self.od.at[layer_of(c), lax.rem(c, CHUNKS), y, z]

    def ex(self, c, i, to):
        return self.copy(self.owner_sem("ex", c) + i, self.nd, self.dblock(c, self.y, self.z), self.at(x=to))

    def placed_down(self, c):
        return pltpu.make_async_copy(self.nd, self.dblock(c, self.y, self.z), self.lsem.at[2, 0])

    def d9(self, c):
        arrive(self.dy2(c))
        k = lax.rem(c, 2)
        for h in PAIR:
            self.xo[:, part(h, HD)] = self.kdy[h, 0] + f32(self.rdy2[k, h])
        self.xb[...] = b16(self.xo[...])

        @pl.when(self.away(c) > 0)
        def _():
            self.dx(c).start()

        leave(self.dy2(c))

    def d10(self, c):
        l = layer_of(c)

        @pl.when(self.away(c) > 0)
        def _():
            self.dx(c).wait_send()

        @pl.when(self.away(c) == 0)
        def _():
            for i in range(1, 4):
                self.dx_in(c, i).wait_recv()
            g = self.xo[...]
            for i in range(3):
                g = g + f32(self.fx[l, i])
            self.nd[...], self.mod[l], self.vod[l] = adamw(f32(self.wd[l]), self.md[l], self.vd[l], f32(b16(g)))
            self.placed_down(c).start()
            for i in range(1, 4):
                self.ex(c, i, self.up_x(i)).start()

    def d11(self, c):
        @pl.when(self.away(c) > 0)
        def _():
            self.ex(c, self.away(c), lax.rem(c, CHUNKS)).wait_recv()

        @pl.when(self.away(c) == 0)
        def _():
            self.placed_down(c).wait()
            for i in range(1, 4):
                self.ex(c, i, self.up_x(i)).wait_send()

        go(self.ey1(c))

    def ey1(self, c, get=False):
        out = []
        for h in PAIR:
            _, q = partners(self.y, h)
            ref = self.dblock(c, q if get else self.y, self.z).at[:, part(h, HD)]
            out.append((ref, ref, self.at(y=q)))
        return self.copies("ey1", c, out)

    def ey2(self, c, get=False):
        out = []
        for h in PAIR:
            first, _ = partners(self.y, h)
            refs = [self.dblock(c, b, self.z).at[:, part(h, HD)] for b in (passed if get else kept)(self.y, h)]
            out += [(ref, ref, self.at(y=first)) for ref in refs]
        return self.copies("ey2", c, out)

    def back(self, c, s, get=False):
        out = []
        for h in PAIR:
            b, to = (self.up_z(s + get), self.up_z(-1)) if h else (self.up_z(-s - get), self.up_z(1))
            ref = self.od.at[layer_of(c), lax.rem(c, CHUNKS), :, b, :, part(h, HD)]
            out.append((ref, ref, self.at(z=to)))
        return self.ringed("back", c, s, out)

    def d12(self, c):
        self.hand_on(self.ey1, self.ey2, c)

    def d13(self, c):
        arrive(self.ey2(c, True))
        go(self.back(c, 0))
        leave(self.ey2(c))

    def ring_back(self, c, s):
        arrive(self.back(c, s - 1, True))
        go(self.back(c, s))
        leave(self.back(c, s - 1))

    def d20(self, c):
        arrive(self.back(c, 6, True))
        leave(self.back(c, 6))


    def weights(self, i):
        l = jnp.where((i >= CHUNKS) & (i < LAST), 1, 0)
        k, ci = lax.rem(i, 2), lax.rem(i, CHUNKS)
        hidden = rows_of(ci, CW)
        pairs = ((self.w_gate.at[l, :, hidden], self.wcg), (self.w_up.at[l, :, hidden], self.wcu), (self.w_down.at[l, hidden], self.wcd))
        return [pltpu.make_async_copy(src, dst.at[k], self.wsem.at[k, i]) for i, (src, dst) in enumerate(pairs)]

    def scale(self, h):
        return lax.rsqrt(jnp.mean(h * h, -1, keepdims=True) + 1e-6)

    def sweep(self, body, n=SUB, lo=0, hi=None):
        def step(t, carry):
            body(rows_of(t, n))
            return carry

        lax.fori_loop(lo, TOK // n if hi is None else hi, step, 0)

    def turn(self, src, dst):
        for i in EIGHT:
            for j in PAIR:
                dst[part(j, SUB), part(i, SUB)] = b16(dot_t(self.eye[...], src[part(i, SUB), part(j, SUB)]))

    def normed(self, rows, h):
        h = f32(h)
        self.a[rows] = b16(h * self.scale(h))

    def start(self):
        i, j = (lax.broadcasted_iota(jnp.int32, (SUB, SUB), axis) for axis in PAIR)
        self.eye[...] = b16(jnp.where(i == j, 1.0, 0.0))
        self.sweep(lambda rows: self.normed(rows, self.xv[rows]))

    def forward(self, i):
        k = lax.rem(i, 2)

        def body(rows):
            a = self.a[rows]
            for n in range(CW // SUB):
                cols = part(n, SUB)
                g = dot(a, self.wcg[k, :, cols])
                u = dot(a, self.wcu[k, :, cols])
                s = 0.5 * jnp.tanh(0.5 * g) + 0.5
                self.act[rows, cols] = b16(g * s * u)
            y = dot(self.act[rows], self.wcd[k])

            @pl.when(i == 0)
            def _():
                self.acc[rows] = y

            @pl.when(i > 0)
            def _():
                self.acc[rows] += y

        self.sweep(body, T)

    def layer_up(self):
        def body(rows):
            h = b16(f32(self.xv[rows]) + f32(b16(self.acc[rows])))
            self.h[rows] = h
            self.normed(rows, h)

        self.sweep(body)
        self.turn(self.a, self.at_)
        self.turn(self.dh, self.dht)

    def layer_down(self):
        def body(rows):
            h = f32(self.h[rows])
            s = self.scale(h)
            ct = f32(b16(self.acc[rows]))
            d = ct * s - h * (s * s * s * jnp.mean(ct * h, -1, keepdims=True))
            self.dh[rows] = b16(f32(self.dh[rows]) + f32(b16(d)))
            self.normed(rows, self.xv[rows])

        self.sweep(body)
        self.turn(self.a, self.at_)
        self.turn(self.dh, self.dht)

    def tiles(self, k, c, lo, hi):
        def body(rows):
            a, dh = self.a[rows], self.dh[rows]
            for n in range(CW // SUB):
                cols = part(n, SUB)
                g = dot(a, self.wcg[k, :, cols])
                u = dot(a, self.wcu[k, :, cols])
                d = f32(b16(dot_t(dh, self.wcd[k, cols])))
                s = 0.5 * jnp.tanh(0.5 * g) + 0.5
                sg = g * s
                self.act[rows, cols] = b16(sg * u)
                self.du[rows, cols] = b16(d * sg)
                self.dg[rows, cols] = b16(d * u * (s + sg * (1.0 - s)))

            @pl.when(c < CHUNKS)
            def _():
                v = dot_t(self.dg[rows], self.wcg[k]) + dot_t(self.du[rows], self.wcu[k])

                @pl.when(c == 0)
                def _():
                    self.acc[rows] = v

                @pl.when(c > 0)
                def _():
                    self.acc[rows] += v

        self.sweep(body, T, lo, hi)

    def grads_down(self, k):
        for n in range(CW // SUB):
            v = dot_t(self.eye[...], b16(dot(self.dht[...], self.act[:, part(n, SUB)])))
            for i in range(SUB // 8):
                q, o = divmod(n * SUB + i * 8, 24)
                self.db[k, q // 8, q % 8, o : o + 8, :] = b16(v[i * 8 : i * 8 + 8])

    def grads(self, k, n):
        cols = part(n, SUB)
        for src, dst in ((self.dg, self.gb), (self.du, self.ub)):
            dst[k, :, :, :, cols] = b16(dot(self.at_[...], src[:, cols])).reshape(*GU, SUB)


def vm(*shape, dtype=BF16):
    return pltpu.VMEM(shape, dtype)


GU = (4, 4, 32)
DN = (4, 8, 24, D)
SCRATCH = dict(
    xv=vm(TOK, D), h=vm(TOK, D), a=vm(TOK, D), at_=vm(D, TOK), dh=vm(TOK, D), dht=vm(D, TOK), acc=vm(TOK, D, dtype=F32),
    act=vm(TOK, CW), dg=vm(TOK, CW), du=vm(TOK, CW), eye=vm(SUB, SUB), wcg=vm(2, D, CW), wcu=vm(2, D, CW), wcd=vm(2, CW, D),
    gb=vm(2, *GU, CW), ub=vm(2, *GU, CW), db=vm(2, *DN),
    r1=vm(2, 2, 2, 2, 4, 32, HW), s2=vm(2, 2, 4, 32, HW), r2=vm(2, 2, 2, 4, 32, HW),
    s3=vm(2, 2, 2, 32, HW), r3=vm(2, 2, 2, 2, 32, HW), keep=vm(2, 2, 2, 32, HW, dtype=F32), s4=vm(2, 2, 32, HW), r4=vm(2, 2, 2, 32, HW),
    zf=vm(8, 2, 2, 4, HW, dtype=F32), zs=vm(8, 2, 2, 4, HW), zo=vm(2, 2, 4, HW, dtype=F32), fz=vm(7, 2, 2, 4, HW),
    nb=vm(2, 2, 4, HW), wz=vm(8, 2, 2, 4, HW), slabf=vm(2, 2, 32, HW, dtype=F32), slab=vm(2, 2, 32, HW),
    rz=vm(2, 2, 7, 4, 24, HD), sdy1=vm(2, 2, 24, HD), rdy1=vm(2, 2, 2, 24, HD), kdy=vm(2, 2, 24, HD, dtype=F32), sdy2=vm(2, 24, HD),
    rdy2=vm(2, 2, 24, HD), xb=vm(24, D), xo=vm(24, D, dtype=F32), fx=vm(2, 3, 24, D), nd=vm(24, D),
    ssem=pltpu.SemaphoreType.DMA((SEMS,)), rsem=pltpu.SemaphoreType.DMA((SEMS,)), lsem=pltpu.SemaphoreType.DMA((3, 2)),
    wsem=pltpu.SemaphoreType.DMA((2, 3)), xsem=pltpu.SemaphoreType.DMA((2,)),
)
HBM_IN = ("x_in", "dy", "w_gate", "w_up", "w_down")
VMEM_IN = ("wg", "wu", "wd", "mg", "mu", "md", "vg", "vu", "vd")
OUT = ("og", "ou", "od", "mog", "mou", "mod", "vog", "vou", "vod")

SLOTS = 8
RINGS = range(1, 7)
EVENTS = {"d0": 4, "w1": 7, "w2": 10, "w3": 12, "w4": 14, "w5": 16, "d7": 18, "w6": 18, "d8": 20, "w7": 20, "d9": 22, "w8": 22}
EVENTS |= {"d10": 24, "w9": 24, "d11": 26, "w10": 27, "d12": 28, "d13": 30, "w11": 30, "d20": 44}
EVENTS |= {("turn_ring", s): 4 + 2 * s for s in RINGS} | {("ring_back", s): 30 + 2 * s for s in RINGS}
SPAN = max(EVENTS.values()) // SLOTS


def kernel(*refs):
    names = HBM_IN + VMEM_IN + OUT + tuple(SCRATCH)
    q = Step(dict(zip(names, refs, strict=True)))
    first = [pltpu.make_async_copy(src.at[0], dst, q.xsem.at[i]) for i, (src, dst) in enumerate(((q.x_in, q.xv), (q.dy, q.dh)))]
    go(first + q.weights(0))
    q.barrier()
    first[0].wait()
    q.start()

    def forward(i, carry):
        go(q.weights(i + 1))
        for w in q.weights(i):
            w.wait()
        q.forward(i)
        return carry

    lax.fori_loop(0, CHUNKS, forward, 0)
    first[1].wait()
    q.layer_up()

    def chunk(c, carry):
        k = lax.rem(c, 2)

        @pl.when(c < LAST - 1)
        def _():
            go(q.weights(c + CHUNKS + 1))

        @pl.when(c < LAST)
        def _():
            for w in q.weights(c + CHUNKS):
                w.wait()

        @pl.when(c == CHUNKS)
        def _():
            q.layer_down()

        pieces = [lambda t=t: q.tiles(k, c, t, t + 1) for t in FOUR] + [lambda: q.grads_down(k)] + [lambda n=n: q.grads(k, n) for n in range(CW // SUB)]
        for slot, piece in enumerate(pieces):

            @pl.when(c < LAST)
            def _():
                run("compute", piece)

            for event, place in sorted(EVENTS.items(), key=lambda item: -item[1]):
                if place % SLOTS == slot:
                    back = place // SLOTS

                    @pl.when((c >= back) & (c < LAST + back))
                    def _():
                        name, args = (event, ()) if isinstance(event, str) else (event[0], event[1:])
                        run(name, getattr(q, name), c - back, *args)

        return carry

    lax.fori_loop(0, LAST + SPAN, chunk, 0)


def run(name, f, *args):
    f(*args)


def solution(mesh):
    def local(x, dy, wg, wu, wd, *mv):
        d = lax.axis_index("dp")
        blocks = [lax.dynamic_slice_in_dim(w, d * n, n, 1) for w, n in ((wg, 4), (wu, 4), (wd, 24))]
        hbm, vmem = (pl.BlockSpec(memory_space=s) for s in (pl.ANY, pltpu.VMEM))
        news = [jax.ShapeDtypeStruct((2, *s), BF16) for s in ((*GU, FF), (*GU, FF), (4, *DN))]
        moments = [jax.ShapeDtypeStruct(t.shape, F32) for t in mv]
        out = pl.pallas_call(
            kernel,
            name="step",
            out_shape=news + moments,
            in_specs=[hbm] * 5 + [vmem] * 9,
            out_specs=[hbm] * 3 + [vmem] * 6,
            scratch_shapes=list(SCRATCH.values()),
            compiler_params=pltpu.CompilerParams(collective_id=1, has_side_effects=True, vmem_limit_bytes=67043328),
        )(x, dy, wg, wu, wd, *blocks, *mv)
        return *(t.reshape(w.shape) for t, w in zip(out, (wg, wu, wd))), *out[3:]

    rows, whole = P(None, "dp", None), P()
    return jax.shard_map(
        local,
        mesh=mesh,
        in_specs=(P(("rep", "dp"), None, None),) * 2 + (whole,) * 3 + (rows,) * 6,
        out_specs=(P("rep", None, None),) * 3 + (P("rep", "dp", None),) * 6,
        check_vma=False,
    )
```

```python
import jax
import jax.numpy as jnp
from jax import lax
from jax.experimental import pallas as pl
from jax.experimental.pallas import tpu as pltpu
from jax.sharding import PartitionSpec as P

MESH = pl.DeviceIdType.MESH
F32, BF16 = jnp.float32, jnp.bfloat16
TOK, D, FF = 2048, 512, 3072
CW = 768
HW = CW // 2
HF = FF // 2
HD = D // 2
LN = 128
CHUNKS = FF // CW
LAST = 2 * CHUNKS
PAIR = (0, 1)
FOUR = range(4)
EIGHT = range(8)
T = 512
SUB = 256


def f32(v):
    return v.astype(F32)


def b16(v):
    return v.astype(BF16)


def dot(a, b):
    return jnp.dot(a, b, preferred_element_type=F32)


def dot_t(a, b):
    return lax.dot_general(a, b, (((1,), (1,)), ((), ())), preferred_element_type=F32)


def rows_of(t, n):
    return pl.ds(pl.multiple_of(t * n, n), n)


def part(i, n):
    return pl.ds(i * n, n)


def flip(p):
    return p + 1 - 2 * lax.rem(p, 2)


def mirror(p):
    return 3 - p


def partners(p, half):
    return (mirror(p), flip(p)) if half else (flip(p), mirror(p))


def passed(p, half):
    first, _ = partners(p, half)
    return first, partners(first, half)[1]


def kept(p, half):
    return p, partners(p, half)[1]


def layer_of(c):
    return jnp.where(c < CHUNKS, 1, 0)


def go(copies):
    for c in copies:
        c.start()


def arrive(copies):
    for c in copies:
        c.wait_recv()


def leave(copies):
    for c in copies:
        c.wait_send()


def adamw(w, m, v, g):
    m = 0.9 * m + 0.1 * g
    v = 0.95 * v + 0.05 * g * g
    step = m * lax.rsqrt(v + 1e-8) + 0.1 * w
    return b16(w - 0.02 * step), m, v


COUNTS = dict(c1=8, c2=4, c3=6, cf=7, a0=7, a1=6, a3=4, a4=8, r0=2, r1=4, r2=2, r3=2, dy=3, dx=3, ex=3, ey=3, b0=2, b1=2, b2=2, b3=2)
FIRST = {}
SEMS = 0
for _name, _n in COUNTS.items():
    FIRST[_name] = SEMS
    SEMS += 2 * _n
OTHERS = (1, 2, 3)


class Step:
    def __init__(self, refs):
        self.__dict__.update(refs)
        d = lax.axis_index("dp")
        self.rep = lax.axis_index("rep")
        self.x, self.y, self.z = d // 32, lax.rem(d // 8, 4), lax.rem(d, 8)


    def at(self, x=None, y=None, z=None):
        x = self.x if x is None else x
        y = self.y if y is None else y
        z = self.z if z is None else z
        return (self.rep, x * 32 + y * 8 + z)

    def up_z(self, i):
        return lax.rem(self.z + i + 16, 8)

    def up_x(self, i):
        return lax.rem(self.x + i + 4, 4)

    def up_y(self, i):
        return lax.rem(self.y + i + 4, 4)

    def up_inner(self, w, i):
        return self.up_x(i) if w else self.up_y(i)

    def copy(self, sem, src, dst, dev):
        return pltpu.make_async_remote_copy(
            src_ref=src, dst_ref=dst, send_sem=self.ssem.at[sem], recv_sem=self.rsem.at[sem], device_id=dev, device_id_type=MESH
        )

    def copies(self, name, c, moves):
        base = FIRST[name] + lax.rem(c, 2) * COUNTS[name]
        return [self.copy(base + i, *move) for i, move in enumerate(moves)]

    def peers(self):
        out = [self.at(z=self.up_z(i)) for i in range(1, 8)]
        return out + [self.at(x=self.up_x(i)) for i in OTHERS] + [self.at(y=self.up_y(i)) for i in OTHERS]

    def greet(self):
        b = pltpu.get_barrier_semaphore()
        for q in self.peers():
            pl.semaphore_signal(b, inc=1, device_id=q, device_id_type=MESH)

    def greeted(self):
        pl.semaphore_wait(pltpu.get_barrier_semaphore(), len(self.peers()))


    def outer(self, w):
        return self.y if w else self.x

    def inner(self, w):
        return self.x if w else self.y

    def at_outer(self, w, p):
        return self.at(y=p) if w else self.at(x=p)

    def at_inner(self, w, p):
        return self.at(x=p) if w else self.at(y=p)

    def halves(self):
        return [(w, h) for w in PAIR for h in PAIR]

    def block(self, w, k, b, h):
        cols = part(h, HW)
        return self.ub.at[k, :, b, :, cols] if w else self.gb.at[k, b, :, :, cols]

    def own(self, w, k, b, j, h):
        cols = part(h, HW)
        return f32(self.ub[k, j, b, :, cols] if w else self.gb[k, b, j, :, cols])

    def c1(self, c):
        k, out = lax.rem(c, 2), []
        for w, h in self.halves():
            first, _ = partners(self.outer(w), h)
            for i, b in enumerate(passed(self.outer(w), h)):
                out.append((self.block(w, k, b, h), self.r1.at[w, k, h, i], self.at_outer(w, first)))
        return self.copies("c1", c, out)

    def c2(self, c):
        k = lax.rem(c, 2)
        return self.copies("c2", c, [(self.s2.at[w, h], self.r2.at[w, k, h], self.at_outer(w, partners(self.outer(w), h)[1])) for w, h in self.halves()])

    def c3(self, c):
        k, out = lax.rem(c, 2), []
        for w in PAIR:
            for i in OTHERS:
                j = self.up_inner(w, i)
                out.append((self.s3.at[w, j], self.r3.at[w, k, i - 1], self.at_inner(w, j)))
        return self.copies("c3", c, out)

    def cf(self, c):
        zs = [self.up_z(i) for i in range(1, 8)]
        return self.copies("cf", c, [(self.zs.at[z], self.fz.at[i], self.at(z=z)) for i, z in enumerate(zs)])

    def w1(self, c):
        go(self.c1(c))

    def w2(self, c):
        arrive(self.c1(c))
        k = lax.rem(c, 2)
        for w, h in self.halves():
            _, b = partners(self.outer(w), h)
            for j in FOUR:
                self.s2[w, h, j] = b16(self.own(w, k, b, j, h) + f32(self.r1[w, k, h, 1, j]))
        go(self.c2(c))
        leave(self.c1(c))

    def wi(self, c):
        arrive(self.c2(c))
        k = lax.rem(c, 2)
        for w, h in self.halves():

            def total(j):
                return self.own(w, k, self.outer(w), j, h) + f32(self.r1[w, k, h, 0, j]) + f32(self.r2[w, k, h, j])

            for i in OTHERS:
                j = self.up_inner(w, i)
                self.s3[w, j, h] = b16(total(j))
            self.keep[w, h] = total(self.inner(w))
        go(self.c3(c))
        leave(self.c2(c))

    def wf(self, c):
        arrive(self.c3(c))
        k = lax.rem(c, 2)
        for w, h in self.halves():
            v = self.keep[w, h]
            for i in range(3):
                v = v + f32(self.r3[w, k, i, h])
            for z in EIGHT:
                self.zf[z, w, h] = v[4 * z : 4 * z + 4]
                self.zs[z, w, h] = b16(v[4 * z : 4 * z + 4])
        self.zo[...] = self.zf[self.z]
        go(self.cf(c))
        leave(self.c3(c))

    def renew(self, c):
        arrive(self.cf(c))
        l, ci = layer_of(c), lax.rem(c, CHUNKS)
        for w, h in self.halves():
            wb, m, v, mo, vo = (getattr(self, s + "gu"[w]) for s in ("w", "m", "v", "mo", "vo"))
            g = self.zo[w, h]
            for i in range(7):
                g = g + f32(self.fz[i, w, h])
            cols = rows_of(2 * ci + h, HW)
            new, mo[l, :, cols], vo[l, :, cols] = adamw(f32(wb[l, :, cols]), m[l, :, cols], v[l, :, cols], f32(b16(g)))
            self.nb[w, h] = new
            self.wz[self.z, w, h] = new
        go(self.a0(c))
        leave(self.cf(c))


    def a0(self, c, get=False):
        zs = [self.up_z(-i if get else i) for i in range(1, 8)]
        return self.copies("a0", c, [(self.nb, self.wz.at[z if get else self.z], self.at(z=z)) for z in zs])

    def cols(self, c, h):
        return rows_of(2 * lax.rem(c, CHUNKS) + h, HW)

    def obig(self, w, c, b, h):
        l, cols = layer_of(c), self.cols(c, h)
        return self.ou.at[l, :, b, :, cols] if w else self.og.at[l, b, :, :, cols]

    def orows(self, w, c, b):
        l, cols = layer_of(c), rows_of(lax.rem(c, CHUNKS), CW)
        return self.ou.at[l, b, self.y, :, cols] if w else self.og.at[l, self.x, b, :, cols]

    def a1(self, c, get=False):
        out = []
        for w in PAIR:
            for i in OTHERS:
                j = self.up_inner(w, -i if get else i)
                out.append((self.slab.at[w], self.orows(w, c, j if get else self.inner(w)), self.at_inner(w, j)))
        return self.copies("a1", c, out)

    def placed(self, c):
        return [pltpu.make_async_copy(self.slab.at[w], self.orows(w, c, self.inner(w)), self.lsem.at[w]) for w in PAIR]

    def a3(self, c, get=False):
        out = []
        for w, h in self.halves():
            _, q = partners(self.outer(w), h)
            ref = self.obig(w, c, q if get else self.outer(w), h)
            out.append((ref, ref, self.at_outer(w, q)))
        return self.copies("a3", c, out)

    def a4(self, c, get=False):
        out = []
        for w, h in self.halves():
            first, _ = partners(self.outer(w), h)
            refs = [self.obig(w, c, b, h) for b in (passed if get else kept)(self.outer(w), h)]
            out += [(ref, ref, self.at_outer(w, first)) for ref in refs]
        return self.copies("a4", c, out)

    def gi(self, c):
        arrive(self.a0(c, True))
        for w, h in self.halves():
            for z in EIGHT:
                self.slabf[w, 4 * z : 4 * z + 4, part(h, HW)] = f32(self.wz[z, w, h])
        self.slab[...] = b16(self.slabf[...])
        go(self.a1(c) + self.placed(c))
        leave(self.a0(c))

    def g1(self, c):
        arrive(self.a1(c, True))
        for p in self.placed(c):
            p.wait()
        go(self.a3(c))
        leave(self.a1(c))

    def g2(self, c):
        self.hand_on(self.a3, self.a4, c)

    def gend(self, c):
        arrive(self.a4(c, True))
        leave(self.a4(c))

    def hand_on(self, before, after, c):
        arrive(before(c, True))
        go(after(c))
        leave(before(c))


    def sides(self):
        return enumerate((self.up_z(1), self.up_z(-1)))

    def far(self, side, n):
        return self.up_z(-n if side else n)

    def dgrad(self, c, b, *cols):
        return self.db.at[(lax.rem(c, 3), slice(None), b, slice(None), *cols)]

    def cr0(self, c):
        k = lax.rem(c, 2)
        return self.copies("r0", c, [(self.dgrad(c, self.far(0, 4), part(h, HD)), self.rz0.at[k, h], self.at(z=to)) for h, to in self.sides()])

    def cr1(self, c):
        k, out = lax.rem(c, 2), []
        for h, to in self.sides():
            out.append((self.rz0.at[k, h], self.rz.at[k, 0, h, :, :, part(h, HD)], self.at(z=to)))
            out.append((self.dgrad(c, self.far(h, 3), part(1 - h, HD)), self.rz.at[k, 0, h, :, :, part(1 - h, HD)], self.at(z=to)))
        return self.copies("r1", c, out)

    def cr2(self, c):
        return self.ringed("r2", c, 1)

    def cr3(self, c):
        return self.ringed("r3", c, 2)

    def ringed(self, name, c, s):
        k = lax.rem(c, 2)
        return self.copies(name, c, [(self.rz.at[k, s - 1, h], self.rz.at[k, s, h], self.at(z=to)) for h, to in self.sides()])

    def d0(self, c):
        go(self.cr0(c))

    def d1(self, c):
        arrive(self.cr0(c))
        k = lax.rem(c, 2)
        for h in PAIR:
            own = self.dgrad(c, self.far(h, 3), part(h, HD))
            for j in FOUR:
                self.rz0[k, h, j] = b16(f32(self.rz0[k, h, j]) + f32(own[j]))
        go(self.cr1(c))
        leave(self.cr0(c))

    def d2(self, c):
        self.pass_on(c, self.cr1, self.cr2, 0)

    def d3(self, c):
        self.pass_on(c, self.cr2, self.cr3, 1)

    def pass_on(self, c, before, after, s):
        arrive(before(c))
        k = lax.rem(c, 2)
        for h in PAIR:
            own = self.dgrad(c, self.far(h, 2 - s))
            for j in FOUR:
                self.rz[k, s, h, j] = b16(f32(self.rz[k, s, h, j]) + f32(own[j]))
        go(after(c))
        leave(before(c))

    def cy(self, c):
        k = lax.rem(c, 2)
        ys = [self.up_y(i) for i in OTHERS]
        return self.copies("dy", c, [(self.sdy.at[y], self.rdy.at[k, i], self.at(y=y)) for i, y in enumerate(ys)])

    def dy_sum(self, c):
        arrive(self.cr3(c))
        k = lax.rem(c, 2)

        def total(j):
            return f32(self.rz[k, 2, 0, j]) + f32(self.rz[k, 2, 1, j]) + f32(self.dgrad(c, self.z)[j])

        for i in OTHERS:
            y = self.up_y(i)
            self.sdy[y] = b16(total(y))
        self.kdy[...] = total(self.y)
        go(self.cy(c))
        leave(self.cr3(c))

    def away(self, c):
        return self.up_x(-lax.rem(c, CHUNKS))

    def owner_sem(self, name, c):
        return FIRST[name] + lax.rem(c, 2) * COUNTS[name] - 1

    def to_owner(self, c, i, x):
        return self.copy(self.owner_sem("dx", c) + i, self.xb, self.fx.at[layer_of(c), i - 1], self.at(x=x))

    def dblock(self, c, y):
        return self.od.at[layer_of(c), lax.rem(c, CHUNKS), y, self.z]

    def from_owner(self, c, i, x):
        return self.copy(self.owner_sem("ex", c) + i, self.nd, self.dblock(c, self.y), self.at(x=x))

    def placed_down(self, c):
        return pltpu.make_async_copy(self.nd, self.dblock(c, self.y), self.lsem.at[2])

    def dx(self, c):
        arrive(self.cy(c))
        k = lax.rem(c, 2)
        v = self.kdy[...]
        for i in range(3):
            v = v + f32(self.rdy[k, i])
        self.xo[...] = v
        self.xb[...] = b16(v)

        @pl.when(self.away(c) > 0)
        def _():
            self.to_owner(c, self.away(c), lax.rem(c, CHUNKS)).start()

        leave(self.cy(c))

    def ex(self, c):
        l = layer_of(c)

        @pl.when(self.away(c) > 0)
        def _():
            self.to_owner(c, self.away(c), lax.rem(c, CHUNKS)).wait_send()

        @pl.when(self.away(c) == 0)
        def _():
            g = self.xo[...]
            for i in OTHERS:
                self.to_owner(c, i, self.up_x(i)).wait_recv()
                g = g + f32(self.fx[l, i - 1])
            self.nd[...], self.mod[l], self.vod[l] = adamw(f32(self.wd[l]), self.md[l], self.vd[l], f32(b16(g)))
            self.placed_down(c).start()
            for i in OTHERS:
                self.from_owner(c, i, self.up_x(i)).start()

    def ey(self, c):
        @pl.when(self.away(c) > 0)
        def _():
            self.from_owner(c, self.away(c), lax.rem(c, CHUNKS)).wait_recv()

        @pl.when(self.away(c) == 0)
        def _():
            self.placed_down(c).wait()
            for i in OTHERS:
                self.from_owner(c, i, self.up_x(i)).wait_send()

        go(self.cz(c))

    def cz(self, c, get=False):
        out = []
        for i in OTHERS:
            y = self.up_y(-i if get else i)
            ref = self.dblock(c, y if get else self.y)
            out.append((ref, ref, self.at(y=y)))
        return self.copies("ey", c, out)

    def back(self, name, n, half=False):
        def moves(c, get=False):
            out = []
            for h, to in self.sides():
                ref = self.od.at[layer_of(c), lax.rem(c, CHUNKS), :, self.far(1 - h, n + get)]
                ref = ref.at[:, :, part(h, HD)] if half else ref
                out.append((ref, ref, self.at(z=to)))
            return self.copies(name, c, out)

        return moves

    def b0(self, c):
        arrive(self.cz(c, True))
        go(self.back("b0", 0)(c))
        leave(self.cz(c))

    def b1(self, c):
        self.hand_on(self.back("b0", 0), self.back("b1", 1), c)

    def b2(self, c):
        self.hand_on(self.back("b1", 1), self.back("b2", 2), c)

    def b3(self, c):
        self.hand_on(self.back("b2", 2), self.back("b3", 3, True), c)

    def dend(self, c):
        arrive(self.back("b3", 3, True)(c, True))
        leave(self.back("b3", 3, True)(c))


    def weights(self, i):
        l = jnp.where((i >= CHUNKS) & (i < LAST), 1, 0)
        k, ci = lax.rem(i, 2), lax.rem(i, CHUNKS)
        hidden = rows_of(ci, CW)
        pairs = ((self.w_gate.at[l, :, hidden], self.wcg), (self.w_up.at[l, :, hidden], self.wcu), (self.w_down.at[l, hidden], self.wcd))
        return [pltpu.make_async_copy(src, dst.at[k], self.wsem.at[k, i]) for i, (src, dst) in enumerate(pairs)]

    def scale(self, h):
        return lax.rsqrt(jnp.mean(h * h, -1, keepdims=True) + 1e-6)

    def sweep(self, body, n=SUB, lo=0, hi=None):
        def step(t, carry):
            body(rows_of(t, n))
            return carry

        lax.fori_loop(lo, TOK // n if hi is None else hi, step, 0)

    def turn(self, src, dst):
        for i in EIGHT:
            for j in PAIR:
                dst[part(j, SUB), part(i, SUB)] = b16(dot_t(self.eye[...], src[part(i, SUB), part(j, SUB)]))

    def normed(self, rows, h):
        h = f32(h)
        self.a[rows] = b16(h * self.scale(h))

    def start(self):
        i, j = (lax.broadcasted_iota(jnp.int32, (SUB, SUB), axis) for axis in PAIR)
        self.eye[...] = b16(jnp.where(i == j, 1.0, 0.0))
        self.sweep(lambda rows: self.normed(rows, self.xv[rows]))

    def forward(self, i):
        k = lax.rem(i, 2)

        def body(rows):
            a = self.a[rows]
            for n in range(CW // SUB):
                cols = part(n, SUB)
                g = dot(a, self.wcg[k, :, cols])
                u = dot(a, self.wcu[k, :, cols])
                s = 0.5 * jnp.tanh(0.5 * g) + 0.5
                self.act[k, rows, cols] = b16(g * s * u)
            y = dot(self.act[k, rows], self.wcd[k])

            @pl.when(i == 0)
            def _():
                self.acc[rows] = y

            @pl.when(i > 0)
            def _():
                self.acc[rows] += y

        self.sweep(body, T)

    def layer_up(self):
        def body(rows):
            h = b16(f32(self.xv[rows]) + f32(b16(self.acc[rows])))
            self.h[rows] = h
            self.normed(rows, h)

        self.sweep(body)
        self.turn(self.a, self.at_)
        self.turn(self.dh, self.dht)

    def layer_down(self):
        def body(rows):
            h = f32(self.h[rows])
            s = self.scale(h)
            ct = f32(b16(self.acc[rows]))
            d = ct * s - h * (s * s * s * jnp.mean(ct * h, -1, keepdims=True))
            self.dh[rows] = b16(f32(self.dh[rows]) + f32(b16(d)))
            self.normed(rows, self.xv[rows])

        self.sweep(body)
        self.turn(self.a, self.at_)
        self.turn(self.dh, self.dht)

    def tiles(self, k, c, lo, hi):
        def body(rows):
            a, dh = self.a[rows], self.dh[rows]
            for n in range(CW // SUB):
                cols = part(n, SUB)
                g = dot(a, self.wcg[k, :, cols])
                u = dot(a, self.wcu[k, :, cols])
                d = f32(b16(dot_t(dh, self.wcd[k, cols])))
                s = 0.5 * jnp.tanh(0.5 * g) + 0.5
                sg = g * s
                self.act[k, rows, cols] = b16(sg * u)
                self.du[rows, cols] = b16(d * sg)
                self.dg[rows, cols] = b16(d * u * (s + sg * (1.0 - s)))

            @pl.when(c < CHUNKS)
            def _():
                v = dot_t(self.dg[rows], self.wcg[k]) + dot_t(self.du[rows], self.wcu[k])

                @pl.when(c == 0)
                def _():
                    self.acc[rows] = v

                @pl.when(c > 0)
                def _():
                    self.acc[rows] += v

        self.sweep(body, T, lo, hi)

    def save(self, i):
        return pltpu.make_async_copy(self.act.at[lax.rem(i, 2)], self.saved.at[i], self.asem.at[lax.rem(i, 2)])

    def load(self, c):
        return pltpu.make_async_copy(self.saved.at[c - CHUNKS], self.act.at[lax.rem(c, 2)], self.asem.at[lax.rem(c, 2)])

    def grads_down(self, c):
        k, kd = lax.rem(c, 2), lax.rem(c, 3)
        for n in range(CW // SUB):
            self.tmp[:, part(n, SUB)] = b16(dot(self.dht[...], self.act[k, :, part(n, SUB)]))
        for n in range(CW // SUB):
            v = dot_t(self.eye[...], self.tmp[:, part(n, SUB)])
            for i in range(SUB // 8):
                q, o = divmod(n * SUB + i * 8, 24)
                self.db[kd, q // 8, q % 8, o : o + 8, :] = b16(v[i * 8 : i * 8 + 8])

    def grads(self, k, n):
        cols = part(n, SUB)
        for src, dst in ((self.dg, self.gb), (self.du, self.ub)):
            dst[k, :, :, :, cols] = b16(dot(self.at_[...], src[:, cols])).reshape(*GU, SUB)


def vm(*shape, dtype=BF16):
    return pltpu.VMEM(shape, dtype)


GU = (4, 4, 32)
DN = (4, 8, 24, D)
SCRATCH = dict(
    xv=vm(TOK, D), h=vm(TOK, D), a=vm(TOK, D), at_=vm(D, TOK), dh=vm(TOK, D), dht=vm(D, TOK), acc=vm(TOK, D, dtype=F32),
    act=vm(2, TOK, CW), dg=vm(TOK, CW), du=vm(TOK, CW), eye=vm(SUB, SUB), tmp=vm(D, CW), wcg=vm(2, D, CW), wcu=vm(2, D, CW), wcd=vm(2, CW, D),
    gb=vm(2, *GU, CW), ub=vm(2, *GU, CW), db=vm(3, *DN),
    r1=vm(2, 2, 2, 2, 4, 32, HW), s2=vm(2, 2, 4, 32, HW), r2=vm(2, 2, 2, 4, 32, HW),
    s3=vm(2, 4, 2, 32, HW), r3=vm(2, 2, 3, 2, 32, HW), keep=vm(2, 2, 32, HW, dtype=F32),
    zf=vm(8, 2, 2, 4, HW, dtype=F32), zs=vm(8, 2, 2, 4, HW), zo=vm(2, 2, 4, HW, dtype=F32), fz=vm(7, 2, 2, 4, HW),
    nb=vm(2, 2, 4, HW), wz=vm(8, 2, 2, 4, HW), slabf=vm(2, 32, CW, dtype=F32), slab=vm(2, 32, CW),
    rz0=vm(2, 2, 4, 24, HD), rz=vm(2, 3, 2, 4, 24, D), sdy=vm(4, 24, D), rdy=vm(2, 3, 24, D), kdy=vm(24, D, dtype=F32),
    xb=vm(24, D), xo=vm(24, D, dtype=F32), fx=vm(2, 3, 24, D), nd=vm(24, D),
    ssem=pltpu.SemaphoreType.DMA((SEMS,)), rsem=pltpu.SemaphoreType.DMA((SEMS,)), lsem=pltpu.SemaphoreType.DMA((3,)),
    wsem=pltpu.SemaphoreType.DMA((2, 3)), xsem=pltpu.SemaphoreType.DMA((2,)), asem=pltpu.SemaphoreType.DMA((2,)),
)
HBM_IN = ("x_in", "dy", "w_gate", "w_up", "w_down")
VMEM_IN = ("wg", "wu", "wd", "mg", "mu", "md", "vg", "vu", "vd")
OUT = ("og", "ou", "od", "mog", "mou", "mod", "vog", "vou", "vod", "saved")

SLOTS = 9
EVENTS = dict(
    w1=(8, 8),
    w2=(12, 12),
    wi=(15, 16),
    wf=(19, 19),
    renew=(22, 25),
    gi=(27, 28),
    g1=(33, 37),
    g2=(40, 43),
    gend=(45, 51),
    d0=(5, 0),
    d1=(8, 3),
    d2=(12, 8),
    d3=(15, 12),
    dy_sum=(19, 17),
    dx=(23, 20),
    ex=(26, 24),
    ey=(29, 27),
    b0=(33, 31),
    b1=(38, 37),
    b2=(46, 46),
    b3=(53, 50),
    dend=(56, 58),
)
SPAN = max(p for both in EVENTS.values() for p in both) // SLOTS


def kernel(*refs):
    names = HBM_IN + VMEM_IN + OUT + tuple(SCRATCH)
    q = Step(dict(zip(names, refs, strict=True)))
    first = [pltpu.make_async_copy(src.at[0], dst, q.xsem.at[i]) for i, (src, dst) in enumerate(((q.x_in, q.xv), (q.dy, q.dh)))]
    go(first + q.weights(0))
    q.greet()
    first[0].wait()
    q.start()

    def forward(i, carry):
        go(q.weights(i + 1))
        for w in q.weights(i):
            w.wait()

        @pl.when(i >= 2)
        def _():
            q.save(i - 2).wait()

        run("forward", q.forward, i)
        q.save(i).start()
        return carry

    lax.fori_loop(0, CHUNKS, forward, 0)
    first[1].wait()
    run("layer_up", q.layer_up)
    for i in (CHUNKS - 2, CHUNKS - 1):
        q.save(i).wait()
    run("greeted", q.greeted)

    def chunk(c, carry):
        k = lax.rem(c, 2)

        @pl.when(c < LAST - 1)
        def _():
            go(q.weights(c + CHUNKS + 1))

        @pl.when((c >= CHUNKS - 1) & (c < LAST - 1))
        def _():
            q.load(c + 1).start()

        @pl.when(c < LAST)
        def _():
            for w in q.weights(c + CHUNKS):
                w.wait()

        @pl.when(c == CHUNKS)
        def _():
            run("layer_down", q.layer_down)

        def down():
            q.load(c).wait()
            q.grads_down(c)

        second, first_ = c < CHUNKS, (c >= CHUNKS) & (c < LAST)
        pieces = [(first_, down)] + [(c < LAST, lambda t=t: q.tiles(k, c, t, t + 1)) for t in FOUR] + [(second, lambda: q.grads_down(c))]
        pieces += [(c < LAST, lambda n=n: q.grads(k, n)) for n in range(CW // SUB)]
        for slot, (when, piece) in enumerate(pieces):

            @pl.when(when)
            def _():
                run("compute", piece)

            due = []
            for event, (second_at, first_at) in EVENTS.items():
                if second_at == first_at:
                    due.append((second_at, 0, LAST, event))
                else:
                    due += [(second_at, 0, CHUNKS, event), (first_at, CHUNKS, LAST, event)]
            for at, lo, hi, event in sorted(due, reverse=True):
                if at % SLOTS == slot:
                    back = at // SLOTS

                    @pl.when((c >= back + lo) & (c < back + hi))
                    def _():
                        run(event, getattr(q, event), c - back)

        return carry

    lax.fori_loop(0, LAST + SPAN, chunk, 0)


def run(name, f, *args):
    f(*args)


def solution(mesh):
    def local(x, dy, wg, wu, wd, *mv):
        d = lax.axis_index("dp")
        blocks = [lax.dynamic_slice_in_dim(w, d * n, n, 1) for w, n in ((wg, 4), (wu, 4), (wd, 24))]
        hbm, vmem = (pl.BlockSpec(memory_space=s) for s in (pl.ANY, pltpu.VMEM))
        news = [jax.ShapeDtypeStruct((2, *s), BF16) for s in ((*GU, FF), (*GU, FF), (4, *DN))]
        moments = [jax.ShapeDtypeStruct(t.shape, F32) for t in mv]
        out = pl.pallas_call(
            kernel,
            name="step",
            out_shape=news + moments + [jax.ShapeDtypeStruct((CHUNKS, TOK, CW), BF16)],
            in_specs=[hbm] * 5 + [vmem] * 9,
            out_specs=[hbm] * 3 + [vmem] * 6 + [hbm],
            scratch_shapes=list(SCRATCH.values()),
            compiler_params=pltpu.CompilerParams(collective_id=1, has_side_effects=True, vmem_limit_bytes=67043328),
        )(x, dy, wg, wu, wd, *blocks, *mv)
        return *(t.reshape(w.shape) for t, w in zip(out, (wg, wu, wd))), *out[3:-1]

    rows, whole = P(None, "dp", None), P()
    return jax.shard_map(
        local,
        mesh=mesh,
        in_specs=(P(("rep", "dp"), None, None),) * 2 + (whole,) * 3 + (rows,) * 6,
        out_specs=(P("rep", None, None),) * 3 + (P("rep", "dp", None),) * 6,
        check_vma=False,
    )
```

```python
import jax
import jax.numpy as jnp
from jax import lax
from jax.experimental import pallas as pl
from jax.experimental.pallas import tpu as pltpu
from jax.sharding import PartitionSpec as P

MESH = pl.DeviceIdType.MESH
F32, BF16 = jnp.float32, jnp.bfloat16
TOK, D, FF = 2048, 512, 3072
CW = 768
HW = CW // 2
HF = FF // 2
HD = D // 2
LN = 128
CHUNKS = FF // CW
LAST = 2 * CHUNKS
PAIR = (0, 1)
FOUR = range(4)
EIGHT = range(8)
T = 512
BIG = 1024
SUB = 256
VMEM_MAIN = 47300000


def f32(v):
    return v.astype(F32)


def b16(v):
    return v.astype(BF16)


def dot(a, b):
    return jnp.dot(a, b, preferred_element_type=F32)


def dot_t(a, b):
    return lax.dot_general(a, b, (((1,), (1,)), ((), ())), preferred_element_type=F32)


def rows_of(t, n):
    return pl.ds(pl.multiple_of(t * n, n), n)


def part(i, n):
    return pl.ds(i * n, n)


def flip(p):
    return p + 1 - 2 * lax.rem(p, 2)


def mirror(p):
    return 3 - p


def partners(p, half):
    return (mirror(p), flip(p)) if half else (flip(p), mirror(p))


def passed(p, half):
    first, _ = partners(p, half)
    return first, partners(first, half)[1]


def kept(p, half):
    return p, partners(p, half)[1]


def layer_of(c):
    return jnp.where(c < CHUNKS, 1, 0)


def go(copies):
    for c in copies:
        c.start()


def arrive(copies):
    for c in copies:
        c.wait_recv()


def leave(copies):
    for c in copies:
        c.wait_send()


def adamw(w, m, v, g):
    m = 0.9 * m + 0.1 * g
    v = 0.95 * v + 0.05 * g * g
    step = m * lax.rsqrt(v + 1e-8) + 0.1 * w
    return b16(w - 0.02 * step), m, v


COUNTS = dict(c1=8, c2=4, c3=6, cf=7, a0=7, a1=6, a3=4, a4=8, r0=2, r1=4, r2=2, r3=2, dy=3, dx=3, ex=3, ey=3, b0=2, b1=2, b2=2, b3=2)
FIRST = {}
SEMS = 0
for _name, _n in COUNTS.items():
    FIRST[_name] = SEMS
    SEMS += 2 * _n
OTHERS = (1, 2, 3)


class Step:
    def __init__(self, refs):
        self.__dict__.update(refs)
        d = lax.axis_index("dp")
        self.rep = lax.axis_index("rep")
        self.x, self.y, self.z = d // 32, lax.rem(d // 8, 4), lax.rem(d, 8)


    def at(self, x=None, y=None, z=None):
        x = self.x if x is None else x
        y = self.y if y is None else y
        z = self.z if z is None else z
        return (self.rep, x * 32 + y * 8 + z)

    def up_z(self, i):
        return lax.rem(self.z + i + 16, 8)

    def up_x(self, i):
        return lax.rem(self.x + i + 4, 4)

    def up_y(self, i):
        return lax.rem(self.y + i + 4, 4)

    def up_inner(self, w, i):
        return self.up_x(i) if w else self.up_y(i)

    def copy(self, sem, src, dst, dev):
        return pltpu.make_async_remote_copy(
            src_ref=src, dst_ref=dst, send_sem=self.ssem.at[sem], recv_sem=self.rsem.at[sem], device_id=dev, device_id_type=MESH
        )

    def copies(self, name, c, moves):
        base = FIRST[name] + lax.rem(c, 2) * COUNTS[name]
        return [self.copy(base + i, *move) for i, move in enumerate(moves)]

    def peers(self):
        out = [self.at(z=self.up_z(i)) for i in range(1, 8)]
        return out + [self.at(x=self.up_x(i)) for i in OTHERS] + [self.at(y=self.up_y(i)) for i in OTHERS]

    def greet(self):
        b = pltpu.get_barrier_semaphore()
        for q in self.peers():
            pl.semaphore_signal(b, inc=1, device_id=q, device_id_type=MESH)

    def greeted(self):
        pl.semaphore_wait(pltpu.get_barrier_semaphore(), len(self.peers()))


    def outer(self, w):
        return self.y if w else self.x

    def inner(self, w):
        return self.x if w else self.y

    def at_outer(self, w, p):
        return self.at(y=p) if w else self.at(x=p)

    def at_inner(self, w, p):
        return self.at(x=p) if w else self.at(y=p)

    def halves(self):
        return [(w, h) for w in PAIR for h in PAIR]

    def block(self, w, k, b, h):
        cols = part(h, HW)
        return self.ub.at[k, :, b, :, cols] if w else self.gb.at[k, b, :, :, cols]

    def own(self, w, k, b, j, h):
        cols = part(h, HW)
        return f32(self.ub[k, j, b, :, cols] if w else self.gb[k, b, j, :, cols])

    def c1(self, c):
        k, out = lax.rem(c, 2), []
        for w, h in self.halves():
            first, _ = partners(self.outer(w), h)
            for i, b in enumerate(passed(self.outer(w), h)):
                out.append((self.block(w, k, b, h), self.r1.at[w, k, h, i], self.at_outer(w, first)))
        return self.copies("c1", c, out)

    def c2(self, c):
        k = lax.rem(c, 2)
        return self.copies("c2", c, [(self.s2.at[w, h], self.r2.at[w, k, h], self.at_outer(w, partners(self.outer(w), h)[1])) for w, h in self.halves()])

    def c3(self, c):
        k, out = lax.rem(c, 2), []
        for w in PAIR:
            for i in OTHERS:
                j = self.up_inner(w, i)
                out.append((self.s3.at[w, j], self.r3.at[w, k, i - 1], self.at_inner(w, j)))
        return self.copies("c3", c, out)

    def cf(self, c):
        zs = [self.up_z(i) for i in range(1, 8)]
        return self.copies("cf", c, [(self.zs.at[z], self.fz.at[i], self.at(z=z)) for i, z in enumerate(zs)])

    def w1(self, c):
        go(self.c1(c))

    def w2(self, c):
        arrive(self.c1(c))
        k = lax.rem(c, 2)
        for w, h in self.halves():
            _, b = partners(self.outer(w), h)
            for j in FOUR:
                self.s2[w, h, j] = b16(self.own(w, k, b, j, h) + f32(self.r1[w, k, h, 1, j]))
        go(self.c2(c))
        leave(self.c1(c))

    def wi(self, c):
        arrive(self.c2(c))
        k = lax.rem(c, 2)
        for w, h in self.halves():

            def total(j):
                return self.own(w, k, self.outer(w), j, h) + f32(self.r1[w, k, h, 0, j]) + f32(self.r2[w, k, h, j])

            for i in OTHERS:
                j = self.up_inner(w, i)
                self.s3[w, j, h] = b16(total(j))
            self.keep[w, h] = total(self.inner(w))
        go(self.c3(c))
        leave(self.c2(c))

    def wf(self, c):
        arrive(self.c3(c))
        k = lax.rem(c, 2)
        for w, h in self.halves():
            v = self.keep[w, h]
            for i in range(3):
                v = v + f32(self.r3[w, k, i, h])
            for z in EIGHT:
                self.zf[z, w, h] = v[4 * z : 4 * z + 4]
                self.zs[z, w, h] = b16(v[4 * z : 4 * z + 4])
        self.zo[...] = self.zf[self.z]
        go(self.cf(c))
        leave(self.c3(c))

    def renew(self, c):
        arrive(self.cf(c))
        l, ci = layer_of(c), lax.rem(c, CHUNKS)
        for w, h in self.halves():
            wb, m, v, mo, vo = (getattr(self, s + "gu"[w]) for s in ("w", "m", "v", "mo", "vo"))
            g = self.zo[w, h]
            for i in range(7):
                g = g + f32(self.fz[i, w, h])
            cols = rows_of(2 * ci + h, HW)
            new, mo[l, :, cols], vo[l, :, cols] = adamw(f32(wb[l, :, cols]), m[l, :, cols], v[l, :, cols], f32(b16(g)))
            self.nb[w, h] = new
            self.wz[self.z, w, h] = new
        go(self.a0(c))
        leave(self.cf(c))


    def a0(self, c, get=False):
        zs = [self.up_z(-i if get else i) for i in range(1, 8)]
        return self.copies("a0", c, [(self.nb, self.wz.at[z if get else self.z], self.at(z=z)) for z in zs])

    def cols(self, c, h):
        return rows_of(2 * lax.rem(c, CHUNKS) + h, HW)

    def obig(self, w, c, b, h):
        l, cols = layer_of(c), self.cols(c, h)
        return self.ou.at[l, :, b, :, cols] if w else self.og.at[l, b, :, :, cols]

    def orows(self, w, c, b):
        l, cols = layer_of(c), rows_of(lax.rem(c, CHUNKS), CW)
        return self.ou.at[l, b, self.y, :, cols] if w else self.og.at[l, self.x, b, :, cols]

    def a1(self, c, get=False):
        out = []
        for w in PAIR:
            for i in OTHERS:
                j = self.up_inner(w, -i if get else i)
                ref = self.orows(w, c, j if get else self.inner(w))
                out.append((ref, ref, self.at_inner(w, j)))
        return self.copies("a1", c, out)

    def a3(self, c, get=False):
        out = []
        for w, h in self.halves():
            _, q = partners(self.outer(w), h)
            ref = self.obig(w, c, q if get else self.outer(w), h)
            out.append((ref, ref, self.at_outer(w, q)))
        return self.copies("a3", c, out)

    def a4(self, c, get=False):
        out = []
        for w, h in self.halves():
            first, _ = partners(self.outer(w), h)
            refs = [self.obig(w, c, b, h) for b in (passed if get else kept)(self.outer(w), h)]
            out += [(ref, ref, self.at_outer(w, first)) for ref in refs]
        return self.copies("a4", c, out)

    def gi(self, c):
        arrive(self.a0(c, True))
        for w in PAIR:
            for h in PAIR:
                for z in EIGHT:
                    self.slab[w, 4 * z : 4 * z + 4, part(h, HW)] = f32(self.wz[z, w, h])
            self.orows(w, c, self.inner(w))[...] = b16(self.slab[w])
        go(self.a1(c))
        leave(self.a0(c))

    def g1(self, c):
        arrive(self.a1(c, True))
        go(self.a3(c))
        leave(self.a1(c))

    def g2(self, c):
        self.hand_on(self.a3, self.a4, c)

    def gend(self, c):
        arrive(self.a4(c, True))
        leave(self.a4(c))

    def hand_on(self, before, after, c):
        arrive(before(c, True))
        go(after(c))
        leave(before(c))


    def sides(self):
        return enumerate((self.up_z(1), self.up_z(-1)))

    def far(self, side, n):
        return self.up_z(-n if side else n)

    def dgrad(self, c, b, *cols):
        return self.db.at[(lax.rem(c, 3), slice(None), b, slice(None), *cols)]

    def cr0(self, c):
        k = lax.rem(c, 2)
        return self.copies("r0", c, [(self.dgrad(c, self.far(0, 4), part(h, HD)), self.rz0.at[k, h], self.at(z=to)) for h, to in self.sides()])

    def cr1(self, c):
        k, out = lax.rem(c, 2), []
        for h, to in self.sides():
            out.append((self.rz0.at[k, h], self.rz.at[k, 0, h, :, :, part(h, HD)], self.at(z=to)))
            out.append((self.dgrad(c, self.far(h, 3), part(1 - h, HD)), self.rz.at[k, 0, h, :, :, part(1 - h, HD)], self.at(z=to)))
        return self.copies("r1", c, out)

    def cr2(self, c):
        return self.ringed("r2", c, 1)

    def cr3(self, c):
        return self.ringed("r3", c, 2)

    def ringed(self, name, c, s):
        k = lax.rem(c, 2)
        return self.copies(name, c, [(self.rz.at[k, s - 1, h], self.rz.at[k, s, h], self.at(z=to)) for h, to in self.sides()])

    def d0(self, c):
        go(self.cr0(c))

    def d1(self, c):
        arrive(self.cr0(c))
        k = lax.rem(c, 2)
        for h in PAIR:
            own = self.dgrad(c, self.far(h, 3), part(h, HD))
            for j in FOUR:
                self.rz0[k, h, j] = b16(f32(self.rz0[k, h, j]) + f32(own[j]))
        go(self.cr1(c))
        leave(self.cr0(c))

    def d2(self, c):
        self.pass_on(c, self.cr1, self.cr2, 0)

    def d3(self, c):
        self.pass_on(c, self.cr2, self.cr3, 1)

    def pass_on(self, c, before, after, s):
        arrive(before(c))
        k = lax.rem(c, 2)
        for h in PAIR:
            own = self.dgrad(c, self.far(h, 2 - s))
            for j in FOUR:
                self.rz[k, s, h, j] = b16(f32(self.rz[k, s, h, j]) + f32(own[j]))
        go(after(c))
        leave(before(c))

    def cy(self, c):
        k = lax.rem(c, 2)
        ys = [self.up_y(i) for i in OTHERS]
        return self.copies("dy", c, [(self.sdy.at[y], self.rdy.at[k, i], self.at(y=y)) for i, y in enumerate(ys)])

    def dy_sum(self, c):
        arrive(self.cr3(c))
        k = lax.rem(c, 2)

        def total(j):
            return f32(self.rz[k, 2, 0, j]) + f32(self.rz[k, 2, 1, j]) + f32(self.dgrad(c, self.z)[j])

        for i in OTHERS:
            y = self.up_y(i)
            self.sdy[y] = b16(total(y))
        self.kdy[...] = total(self.y)
        go(self.cy(c))
        leave(self.cr3(c))

    def away(self, c):
        return self.up_x(-lax.rem(c, CHUNKS))

    def owner_sem(self, name, c):
        return FIRST[name] + lax.rem(c, 2) * COUNTS[name] - 1

    def to_owner(self, c, i, x):
        return self.copy(self.owner_sem("dx", c) + i, self.xb, self.fx.at[layer_of(c), i - 1], self.at(x=x))

    def dblock(self, c, y):
        return self.od.at[layer_of(c), lax.rem(c, CHUNKS), y, self.z]

    def from_owner(self, c, i, x):
        ref = self.dblock(c, self.y)
        return self.copy(self.owner_sem("ex", c) + i, ref, ref, self.at(x=x))

    def dx(self, c):
        arrive(self.cy(c))
        k = lax.rem(c, 2)
        v = self.kdy[...]
        for i in range(3):
            v = v + f32(self.rdy[k, i])
        self.xo[...] = v
        self.xb[...] = b16(v)

        @pl.when(self.away(c) > 0)
        def _():
            self.to_owner(c, self.away(c), lax.rem(c, CHUNKS)).start()

        leave(self.cy(c))

    def ex(self, c):
        l = layer_of(c)

        @pl.when(self.away(c) > 0)
        def _():
            self.to_owner(c, self.away(c), lax.rem(c, CHUNKS)).wait_send()

        @pl.when(self.away(c) == 0)
        def _():
            g = self.xo[...]
            for i in OTHERS:
                self.to_owner(c, i, self.up_x(i)).wait_recv()
                g = g + f32(self.fx[l, i - 1])
            self.dblock(c, self.y)[...], self.mod[l], self.vod[l] = adamw(f32(self.wd[l]), self.md[l], self.vd[l], f32(b16(g)))
            for i in OTHERS:
                self.from_owner(c, i, self.up_x(i)).start()

    def ey(self, c):
        @pl.when(self.away(c) > 0)
        def _():
            self.from_owner(c, self.away(c), lax.rem(c, CHUNKS)).wait_recv()

        @pl.when(self.away(c) == 0)
        def _():
            for i in OTHERS:
                self.from_owner(c, i, self.up_x(i)).wait_send()

        go(self.cz(c))

    def cz(self, c, get=False):
        out = []
        for i in OTHERS:
            y = self.up_y(-i if get else i)
            ref = self.dblock(c, y if get else self.y)
            out.append((ref, ref, self.at(y=y)))
        return self.copies("ey", c, out)

    def back(self, name, n, half=False):
        def moves(c, get=False):
            out = []
            for h, to in self.sides():
                ref = self.od.at[layer_of(c), lax.rem(c, CHUNKS), :, self.far(1 - h, n + get)]
                ref = ref.at[:, :, part(h, HD)] if half else ref
                out.append((ref, ref, self.at(z=to)))
            return self.copies(name, c, out)

        return moves

    def b0(self, c):
        arrive(self.cz(c, True))
        go(self.back("b0", 0)(c))
        leave(self.cz(c))

    def b1(self, c):
        self.hand_on(self.back("b0", 0), self.back("b1", 1), c)

    def b2(self, c):
        self.hand_on(self.back("b1", 1), self.back("b2", 2), c)

    def b3(self, c):
        self.hand_on(self.back("b2", 2), self.back("b3", 3, True), c)

    def dend(self, c):
        arrive(self.back("b3", 3, True)(c, True))
        leave(self.back("b3", 3, True)(c))


    def weights(self, i):
        l = jnp.where((i >= CHUNKS) & (i < LAST), 1, 0)
        k, ci = lax.rem(i, 2), lax.rem(i, CHUNKS)
        hidden = rows_of(ci, CW)
        pairs = ((self.w_gate.at[l, :, hidden], self.wcg), (self.w_up.at[l, :, hidden], self.wcu), (self.w_down.at[l, hidden], self.wcd))
        return [pltpu.make_async_copy(src, dst.at[k], self.wsem.at[k, i]) for i, (src, dst) in enumerate(pairs)]

    def scale(self, h):
        return lax.rsqrt(jnp.mean(h * h, -1, keepdims=True) + 1e-6)

    def sweep(self, body, n=SUB, lo=0, hi=None):
        def step(t, carry):
            body(rows_of(t, n))
            return carry

        lax.fori_loop(lo, TOK // n if hi is None else hi, step, 0)

    def turn(self, src, dst):
        for i in EIGHT:
            for j in PAIR:
                dst[part(j, SUB), part(i, SUB)] = b16(dot_t(self.eye[...], src[part(i, SUB), part(j, SUB)]))

    def normed(self, rows, h):
        h = f32(h)
        self.a[rows] = b16(h * self.scale(h))

    def start(self):
        i, j = (lax.broadcasted_iota(jnp.int32, (SUB, SUB), axis) for axis in PAIR)
        self.eye[...] = b16(jnp.where(i == j, 1.0, 0.0))
        self.acc[...] = jnp.zeros_like(self.acc)

    def start_rows(self):
        self.sweep(lambda rows: self.normed(rows, self.xv[rows]), BIG)

    def own_blocks(self):
        tiles = [(l, w, j) for l in PAIR for w in PAIR for j in FOUR]
        rows = rows_of(4 * self.x + self.y, 32)
        refs = (self.w_gate, self.w_up)
        out = [pltpu.make_async_copy(refs[w].at[l, rows, part(j, CW)], self.gb.at[l, w, j], self.osem.at[i]) for i, (l, w, j) in enumerate(tiles)]
        mine = rows_of(32 * self.x + 8 * self.y + self.z, 24)
        return out + [pltpu.make_async_copy(self.w_down.at[l, mine], self.wd.at[l], self.osem.at[len(tiles) + l]) for l in PAIR]

    def pick_rows(self):
        for l in PAIR:
            for j in FOUR:
                for w in PAIR:
                    v = f32(self.gb[l, w, j])
                    for z in EIGHT:
                        for h in PAIR:
                            self.zf[z, w, h] = v[4 * z : 4 * z + 4, h * HW : (h + 1) * HW]
                    for h in PAIR:
                        (self.wu if w else self.wg)[l, :, part(2 * j + h, HW)] = self.zf[self.z, w, h]

    def forward(self, i):
        k = lax.rem(i, 2)

        def tile(t, carry):
            rows = rows_of(t, BIG)

            @pl.when(i > 0)
            def _():
                self.save(i - 1, t).wait()

            a = self.a[rows]
            for n in range(CW // SUB):
                cols = part(n, SUB)
                g = dot(a, self.wcg[k, :, cols])
                u = dot(a, self.wcu[k, :, cols])
                s = 0.5 * jnp.tanh(0.5 * g) + 0.5
                self.act[rows, cols] = b16(g * s * u)
            self.acc[rows] += dot(self.act[rows], self.wcd[k])
            self.save(i, t).start()
            return carry

        lax.fori_loop(0, TOK // BIG, tile, 0)

    def layer_up(self):
        def body(rows):
            h = b16(f32(self.xv[rows]) + f32(b16(self.acc[rows])))
            self.h[rows] = h
            self.normed(rows, h)
            self.acc[rows] = jnp.zeros((SUB, D), F32)

        self.sweep(body)
        self.turn(self.a, self.at_)
        self.turn(self.dh, self.dht)

    def layer_down(self):
        def body(rows):
            h = f32(self.h[rows])
            s = self.scale(h)
            ct = f32(b16(self.acc[rows]))
            d = ct * s - h * (s * s * s * jnp.mean(ct * h, -1, keepdims=True))
            self.dh[rows] = b16(f32(self.dh[rows]) + f32(b16(d)))

        self.sweep(body)
        self.kept_a().wait()
        self.turn(self.a, self.at_)
        self.turn(self.dh, self.dht)

    def tiles(self, k, second, n, t):
        def body(rows):
            a, dh = self.a[rows], self.dh[rows]
            for i in range(CW // SUB):
                cols = part(i, SUB)
                g = dot(a, self.wcg[k, :, cols])
                u = dot(a, self.wcu[k, :, cols])
                d = f32(b16(dot_t(dh, self.wcd[k, cols])))
                s = 0.5 * jnp.tanh(0.5 * g) + 0.5
                sg = g * s
                if second:
                    self.act[rows, cols] = b16(sg * u)
                self.du[rows, cols] = b16(d * sg)
                self.dg[rows, cols] = b16(d * u * (s + sg * (1.0 - s)))
            if second:
                self.acc[rows] += dot_t(self.dg[rows], self.wcg[k]) + dot_t(self.du[rows], self.wcu[k])

        self.sweep(body, n, t, t + 1)

    def save(self, i, t):
        rows = rows_of(t, BIG)
        return pltpu.make_async_copy(self.act.at[rows], self.saved.at[i, rows], self.asem.at[t])

    def load(self, c):
        return pltpu.make_async_copy(self.saved.at[c - CHUNKS], self.act, self.asem.at[0])

    def keep_a(self):
        return pltpu.make_async_copy(self.a, self.saved_a, self.asem.at[2])

    def kept_a(self):
        return pltpu.make_async_copy(self.saved_a, self.a, self.asem.at[2])

    def grads_down(self, c):
        kd = lax.rem(c, 3)
        for n in range(CW // SUB):
            self.tmp[:, part(n, SUB)] = b16(dot(self.dht[...], self.act[:, part(n, SUB)]))
        for n in range(CW // SUB):
            v = dot_t(self.eye[...], self.tmp[:, part(n, SUB)])
            for i in range(SUB // 8):
                q, o = divmod(n * SUB + i * 8, 24)
                self.db[kd, q // 8, q % 8, o : o + 8, :] = b16(v[i * 8 : i * 8 + 8])

    def grads(self, k, w):
        src, dst = (self.du, self.ub) if w else (self.dg, self.gb)
        dst[k] = b16(dot(self.at_[...], src[...])).reshape(*GU, CW)


def vm(*shape, dtype=BF16):
    return pltpu.VMEM(shape, dtype)


GU = (4, 4, 32)
DN = (4, 8, 24, D)
SCRATCH = dict(
    h=vm(TOK, D), a=vm(TOK, D), at_=vm(D, TOK), dh=vm(TOK, D), dht=vm(D, TOK), acc=vm(TOK, D, dtype=F32),
    act=vm(TOK, CW), dg=vm(TOK, CW), du=vm(TOK, CW), eye=vm(SUB, SUB), tmp=vm(D, CW), wcg=vm(2, D, CW), wcu=vm(2, D, CW), wcd=vm(2, CW, D),
    gb=vm(2, *GU, CW), ub=vm(2, *GU, CW), db=vm(3, *DN),
    r1=vm(2, 2, 2, 2, 4, 32, HW), s2=vm(2, 2, 4, 32, HW), r2=vm(2, 2, 2, 4, 32, HW),
    s3=vm(2, 4, 2, 32, HW), r3=vm(2, 2, 3, 2, 32, HW), keep=vm(2, 2, 32, HW, dtype=F32),
    zf=vm(8, 2, 2, 4, HW, dtype=F32), zs=vm(8, 2, 2, 4, HW), zo=vm(2, 2, 4, HW, dtype=F32), fz=vm(7, 2, 2, 4, HW),
    nb=vm(2, 2, 4, HW), wz=vm(8, 2, 2, 4, HW), slab=vm(2, 32, CW, dtype=F32),
    rz0=vm(2, 2, 4, 24, HD), rz=vm(2, 3, 2, 4, 24, D), sdy=vm(4, 24, D), rdy=vm(2, 3, 24, D), kdy=vm(24, D, dtype=F32),
    xb=vm(24, D), xo=vm(24, D, dtype=F32), fx=vm(2, 3, 24, D), wg=vm(2, 4, FF, dtype=F32), wu=vm(2, 4, FF, dtype=F32), wd=vm(2, 24, D),
    ssem=pltpu.SemaphoreType.DMA((SEMS,)), rsem=pltpu.SemaphoreType.DMA((SEMS,)), osem=pltpu.SemaphoreType.DMA((18,)),
    wsem=pltpu.SemaphoreType.DMA((2, 3)), xsem=pltpu.SemaphoreType.DMA((2,)), asem=pltpu.SemaphoreType.DMA((3,)),
)
HBM_IN = ("x_in", "dy", "w_gate", "w_up", "w_down")
VMEM_IN = ("mg", "mu", "md", "vg", "vu", "vd")
OUT = ("og", "ou", "od", "mog", "mou", "mod", "vog", "vou", "vod", "saved", "saved_a")

SLOTS = 8
EVENTS = dict(
    w1=(7, 7),
    w2=(11, 11),
    wi=(14, 14),
    wf=(19, 19),
    renew=(23, 23),
    gi=(27, 27),
    g1=(32, 33),
    g2=(37, 38),
    gend=(42, 46),
    d0=(5, 0),
    d1=(7, 3),
    d2=(11, 8),
    d3=(14, 11),
    dy_sum=(18, 15),
    dx=(20, 18),
    ex=(22, 21),
    ey=(25, 24),
    b0=(30, 28),
    b1=(33, 32),
    b2=(37, 37),
    b3=(41, 42),
    dend=(46, 47),
)
SPAN = max(p for both in EVENTS.values() for p in both) // SLOTS


def kernel(*refs):
    names = HBM_IN + VMEM_IN + OUT + tuple(SCRATCH)
    q = Step(dict(zip(names, refs, strict=True)))
    q.xv = q.dg.at[:, part(0, D)]
    first = [pltpu.make_async_copy(src.at[0], dst, q.xsem.at[i]) for i, (src, dst) in enumerate(((q.x_in, q.xv), (q.dy, q.dh)))]
    go(first + q.weights(0) + q.own_blocks())
    q.greet()
    run("start", q.start)
    first[0].wait()
    run("start_rows", q.start_rows)
    q.keep_a().start()

    def forward(i, carry):
        go(q.weights(i + 1))
        for w in q.weights(i):
            w.wait()

        run("forward", q.forward, i)
        return carry

    lax.fori_loop(0, CHUNKS, forward, 0)
    first[1].wait()
    q.keep_a().wait()
    run("layer_up", q.layer_up)
    for t in PAIR:
        q.save(CHUNKS - 1, t).wait()
    for c in q.own_blocks():
        c.wait()
    run("pick_rows", q.pick_rows)
    run("greeted", q.greeted)

    def chunk(c, carry):
        k = lax.rem(c, 2)

        @pl.when(c < LAST - 1)
        def _():
            go(q.weights(c + CHUNKS + 1))

        @pl.when(c < LAST)
        def _():
            for w in q.weights(c + CHUNKS):
                w.wait()

        @pl.when(c == CHUNKS)
        def _():
            run("layer_down", q.layer_down)

        def down():
            q.load(c).wait()
            q.grads_down(c)

            @pl.when(c < LAST - 1)
            def _():
                q.load(c + 1).start()

        def down_second():
            q.grads_down(c)

            @pl.when(c == CHUNKS - 1)
            def _():
                q.load(c + 1).start()
                q.kept_a().start()

        second, first_, both = c < CHUNKS, (c >= CHUNKS) & (c < LAST), c < LAST
        pieces = {slot: [] for slot in range(SLOTS)}
        pieces[0].append((first_, down))
        for t in FOUR:
            pieces[1 + t].append((second, lambda t=t: q.tiles(k, True, T, t)))
        for t in PAIR:
            pieces[2 + 2 * t].append((first_, lambda t=t: q.tiles(k, False, BIG, t)))
            pieces[6 + t].append((both, lambda t=t: q.grads(k, t)))
        pieces[5].append((second, down_second))
        for slot in range(SLOTS):
            for when, piece in pieces[slot]:

                @pl.when(when)
                def _():
                    run("compute", piece)

            due = []
            for event, (second_at, first_at) in EVENTS.items():
                if second_at == first_at:
                    due.append((second_at, 0, LAST, event))
                else:
                    due += [(second_at, 0, CHUNKS, event), (first_at, CHUNKS, LAST, event)]
            for at, lo, hi, event in sorted(due, reverse=True):
                if at % SLOTS == slot:
                    back = at // SLOTS

                    @pl.when((c >= back + lo) & (c < back + hi))
                    def _():
                        run(event, getattr(q, event), c - back)

        return carry

    lax.fori_loop(0, LAST + SPAN, chunk, 0)


def run(name, f, *args):
    f(*args)


def place(*refs):
    n = len(refs) // 2
    copies = [pltpu.make_async_copy(src, dst, refs[-1].at[i]) for i, (src, dst) in enumerate(zip(refs[:n], refs[n:-1], strict=True))]
    go(copies)
    for c in copies:
        c.wait()


def solution(mesh):
    def local(x, dy, wg, wu, wd, *mv):
        hbm, vmem = (pl.BlockSpec(memory_space=s) for s in (pl.ANY, pltpu.VMEM))
        news = [jax.ShapeDtypeStruct((2, *s), BF16) for s in ((*GU, FF), (*GU, FF), (4, *DN))]
        moments = [jax.ShapeDtypeStruct(t.shape, F32) for t in mv]
        kept = [jax.ShapeDtypeStruct(s, BF16) for s in ((CHUNKS, TOK, CW), (TOK, D))]
        out = pl.pallas_call(
            kernel,
            name="step",
            out_shape=[pltpu.VMEM(t.shape, t.dtype) for t in news + moments] + kept,
            in_specs=[hbm] * 5 + [vmem] * 6,
            out_specs=[vmem] * 9 + [hbm] * 2,
            scratch_shapes=list(SCRATCH.values()),
            compiler_params=pltpu.CompilerParams(collective_id=1, has_side_effects=True, vmem_limit_bytes=VMEM_MAIN),
        )(x, dy, wg, wu, wd, *mv)
        placed = pl.pallas_call(
            place,
            name="place",
            out_shape=news + moments,
            in_specs=[vmem] * 9,
            out_specs=[hbm] * 9,
            scratch_shapes=[pltpu.SemaphoreType.DMA((9,))],
            compiler_params=pltpu.CompilerParams(vmem_limit_bytes=1 << 20),
        )(*out[:9])
        return *(t.reshape(w.shape) for t, w in zip(placed, (wg, wu, wd))), *placed[3:]

    rows, whole = P(None, "dp", None), P()
    return jax.shard_map(
        local,
        mesh=mesh,
        in_specs=(P(("rep", "dp"), None, None),) * 2 + (whole,) * 3 + (rows,) * 6,
        out_specs=(P("rep", None, None),) * 3 + (P("rep", "dp", None),) * 6,
        check_vma=False,
    )
```

```python
import jax
import jax.numpy as jnp
from jax import lax
from jax.experimental import pallas as pl
from jax.experimental.pallas import tpu as pltpu
from jax.sharding import PartitionSpec as P

MESH = pl.DeviceIdType.MESH
F32, BF16 = jnp.float32, jnp.bfloat16
TOK, D, FF = 2048, 512, 3072
CW = 768
HW = CW // 2
HF = FF // 2
HD = D // 2
LN = 128
CHUNKS = FF // CW
LAST = 2 * CHUNKS
PAIR = (0, 1)
FOUR = range(4)
EIGHT = range(8)
T = 512
BIG = 1024
SUB = 256
VMEM_MAIN = 47300000


def f32(v):
    return v.astype(F32)


def b16(v):
    return v.astype(BF16)


def dot(a, b):
    return jnp.dot(a, b, preferred_element_type=F32)


def dot_t(a, b):
    return lax.dot_general(a, b, (((1,), (1,)), ((), ())), preferred_element_type=F32)


def rows_of(t, n):
    return pl.ds(pl.multiple_of(t * n, n), n)


def part(i, n):
    return pl.ds(i * n, n)


def flip(p):
    return p + 1 - 2 * lax.rem(p, 2)


def mirror(p):
    return 3 - p


def partners(p, half):
    return (mirror(p), flip(p)) if half else (flip(p), mirror(p))


def passed(p, half):
    first, _ = partners(p, half)
    return first, partners(first, half)[1]


def kept(p, half):
    return p, partners(p, half)[1]


def layer_of(c):
    return jnp.where(c < CHUNKS, 1, 0)


def go(copies):
    for c in copies:
        c.start()


def arrive(copies):
    for c in copies:
        c.wait_recv()


def leave(copies):
    for c in copies:
        c.wait_send()


def adamw(w, m, v, g):
    m = 0.9 * m + 0.1 * g
    v = 0.95 * v + 0.05 * g * g
    step = m * lax.rsqrt(v + 1e-8) + 0.1 * w
    return b16(w - 0.02 * step), m, v


COUNTS = dict(c1=8, c2=4, c3=6, cf=7, a0=7, a1=6, a3=4, a4=8, r0=2, r1=4, r2=2, r3=2, dy=3, dx=3, ex=3, ey=3, b0=2, b1=2, b2=2, b3=2)
FIRST = {}
SEMS = 0
for _name, _n in COUNTS.items():
    FIRST[_name] = SEMS
    SEMS += 2 * _n
OTHERS = (1, 2, 3)


class Step:
    def __init__(self, refs):
        self.__dict__.update(refs)
        d = lax.axis_index("dp")
        self.rep = lax.axis_index("rep")
        self.x, self.y, self.z = d // 32, lax.rem(d // 8, 4), lax.rem(d, 8)


    def at(self, x=None, y=None, z=None):
        x = self.x if x is None else x
        y = self.y if y is None else y
        z = self.z if z is None else z
        return (self.rep, x * 32 + y * 8 + z)

    def up_z(self, i):
        return lax.rem(self.z + i + 16, 8)

    def up_x(self, i):
        return lax.rem(self.x + i + 4, 4)

    def up_y(self, i):
        return lax.rem(self.y + i + 4, 4)

    def up_inner(self, w, i):
        return self.up_x(i) if w else self.up_y(i)

    def copy(self, sem, src, dst, dev):
        return pltpu.make_async_remote_copy(
            src_ref=src, dst_ref=dst, send_sem=self.ssem.at[sem], recv_sem=self.rsem.at[sem], device_id=dev, device_id_type=MESH
        )

    def copies(self, name, c, moves):
        base = FIRST[name] + lax.rem(c, 2) * COUNTS[name]
        return [self.copy(base + i, *move) for i, move in enumerate(moves)]

    def peers(self):
        out = [self.at(z=self.up_z(i)) for i in range(1, 8)]
        return out + [self.at(x=self.up_x(i)) for i in OTHERS] + [self.at(y=self.up_y(i)) for i in OTHERS]

    def greet(self):
        b = pltpu.get_barrier_semaphore()
        for q in self.peers():
            pl.semaphore_signal(b, inc=1, device_id=q, device_id_type=MESH)

    def greeted(self):
        pl.semaphore_wait(pltpu.get_barrier_semaphore(), len(self.peers()))


    def outer(self, w):
        return self.y if w else self.x

    def inner(self, w):
        return self.x if w else self.y

    def at_outer(self, w, p):
        return self.at(y=p) if w else self.at(x=p)

    def at_inner(self, w, p):
        return self.at(x=p) if w else self.at(y=p)

    def halves(self):
        return [(w, h) for w in PAIR for h in PAIR]

    def block(self, w, k, b, h):
        cols = part(h, HW)
        return self.ub.at[k, :, b, :, cols] if w else self.gb.at[k, b, :, :, cols]

    def own(self, w, k, b, j, h):
        cols = part(h, HW)
        return f32(self.ub[k, j, b, :, cols] if w else self.gb[k, b, j, :, cols])

    def c1(self, c):
        k, out = lax.rem(c, 2), []
        for w, h in self.halves():
            first, _ = partners(self.outer(w), h)
            for i, b in enumerate(passed(self.outer(w), h)):
                out.append((self.block(w, k, b, h), self.r1.at[w, k, h, i], self.at_outer(w, first)))
        return self.copies("c1", c, out)

    def c2(self, c):
        k = lax.rem(c, 2)
        return self.copies("c2", c, [(self.s2.at[w, h], self.r2.at[w, k, h], self.at_outer(w, partners(self.outer(w), h)[1])) for w, h in self.halves()])

    def c3(self, c):
        k, out = lax.rem(c, 2), []
        for w in PAIR:
            for i in OTHERS:
                j = self.up_inner(w, i)
                out.append((self.s3.at[w, j], self.r3.at[w, k, i - 1], self.at_inner(w, j)))
        return self.copies("c3", c, out)

    def cf(self, c):
        zs = [self.up_z(i) for i in range(1, 8)]
        return self.copies("cf", c, [(self.zs.at[z], self.fz.at[i], self.at(z=z)) for i, z in enumerate(zs)])

    def w1(self, c):
        go(self.c1(c))

    def w2(self, c):
        arrive(self.c1(c))
        k = lax.rem(c, 2)
        for w, h in self.halves():
            _, b = partners(self.outer(w), h)
            for j in FOUR:
                self.s2[w, h, j] = b16(self.own(w, k, b, j, h) + f32(self.r1[w, k, h, 1, j]))
        go(self.c2(c))
        leave(self.c1(c))

    def wi(self, c):
        arrive(self.c2(c))
        k = lax.rem(c, 2)
        for w, h in self.halves():

            def total(j):
                return self.own(w, k, self.outer(w), j, h) + f32(self.r1[w, k, h, 0, j]) + f32(self.r2[w, k, h, j])

            for i in OTHERS:
                j = self.up_inner(w, i)
                self.s3[w, j, h] = b16(total(j))
            self.keep[w, h] = total(self.inner(w))
        go(self.c3(c))
        leave(self.c2(c))

    def wf(self, c):
        arrive(self.c3(c))
        k = lax.rem(c, 2)
        for w, h in self.halves():
            v = self.keep[w, h]
            for i in range(3):
                v = v + f32(self.r3[w, k, i, h])
            for z in EIGHT:
                self.zf[z, w, h] = v[4 * z : 4 * z + 4]
                self.zs[z, w, h] = b16(v[4 * z : 4 * z + 4])
        self.zo[...] = self.zf[self.z]
        go(self.cf(c))
        leave(self.c3(c))

    def renew(self, c):
        arrive(self.cf(c))
        l, ci = layer_of(c), lax.rem(c, CHUNKS)
        for w, h in self.halves():
            wb, m, v, mo, vo = (getattr(self, s + "gu"[w]) for s in ("w", "m", "v", "mo", "vo"))
            g = self.zo[w, h]
            for i in range(7):
                g = g + f32(self.fz[i, w, h])
            cols = rows_of(2 * ci + h, HW)
            new, mo[l, :, cols], vo[l, :, cols] = adamw(f32(wb[l, :, cols]), m[l, :, cols], v[l, :, cols], f32(b16(g)))
            self.nb[w, h] = new
            self.wz[self.z, w, h] = new
        go(self.a0(c))
        leave(self.cf(c))


    def a0(self, c, get=False):
        zs = [self.up_z(-i if get else i) for i in range(1, 8)]
        return self.copies("a0", c, [(self.nb, self.wz.at[z if get else self.z], self.at(z=z)) for z in zs])

    def cols(self, c, h):
        return rows_of(2 * lax.rem(c, CHUNKS) + h, HW)

    def obig(self, w, c, b, h):
        l, cols = layer_of(c), self.cols(c, h)
        return self.ou.at[l, :, b, :, cols] if w else self.og.at[l, b, :, :, cols]

    def orows(self, w, c, b):
        l, cols = layer_of(c), rows_of(lax.rem(c, CHUNKS), CW)
        return self.ou.at[l, b, self.y, :, cols] if w else self.og.at[l, self.x, b, :, cols]

    def a1(self, c, get=False):
        out = []
        for w in PAIR:
            for i in OTHERS:
                j = self.up_inner(w, -i if get else i)
                ref = self.orows(w, c, j if get else self.inner(w))
                out.append((ref, ref, self.at_inner(w, j)))
        return self.copies("a1", c, out)

    def a3(self, c, get=False):
        out = []
        for w, h in self.halves():
            _, q = partners(self.outer(w), h)
            ref = self.obig(w, c, q if get else self.outer(w), h)
            out.append((ref, ref, self.at_outer(w, q)))
        return self.copies("a3", c, out)

    def a4(self, c, get=False):
        out = []
        for w, h in self.halves():
            first, _ = partners(self.outer(w), h)
            refs = [self.obig(w, c, b, h) for b in (passed if get else kept)(self.outer(w), h)]
            out += [(ref, ref, self.at_outer(w, first)) for ref in refs]
        return self.copies("a4", c, out)

    def gi(self, c):
        arrive(self.a0(c, True))
        for w in PAIR:
            for h in PAIR:
                for z in EIGHT:
                    self.slab[w, 4 * z : 4 * z + 4, part(h, HW)] = f32(self.wz[z, w, h])
            self.orows(w, c, self.inner(w))[...] = b16(self.slab[w])
        go(self.a1(c))
        leave(self.a0(c))

    def g1(self, c):
        arrive(self.a1(c, True))
        go(self.a3(c))
        leave(self.a1(c))

    def g2(self, c):
        self.hand_on(self.a3, self.a4, c)

    def gend(self, c):
        arrive(self.a4(c, True))
        leave(self.a4(c))

    def hand_on(self, before, after, c):
        arrive(before(c, True))
        go(after(c))
        leave(before(c))


    def sides(self):
        return enumerate((self.up_z(1), self.up_z(-1)))

    def far(self, side, n):
        return self.up_z(-n if side else n)

    def dgrad(self, c, b, *cols):
        return self.db.at[(lax.rem(c, 3), slice(None), b, slice(None), *cols)]

    def cr0(self, c):
        k = lax.rem(c, 2)
        return self.copies("r0", c, [(self.dgrad(c, self.far(0, 4), part(h, HD)), self.rz0.at[k, h], self.at(z=to)) for h, to in self.sides()])

    def cr1(self, c):
        k, out = lax.rem(c, 2), []
        for h, to in self.sides():
            out.append((self.rz0.at[k, h], self.rz.at[k, 0, h, :, :, part(h, HD)], self.at(z=to)))
            out.append((self.dgrad(c, self.far(h, 3), part(1 - h, HD)), self.rz.at[k, 0, h, :, :, part(1 - h, HD)], self.at(z=to)))
        return self.copies("r1", c, out)

    def cr2(self, c):
        return self.ringed("r2", c, 1)

    def cr3(self, c):
        return self.ringed("r3", c, 2)

    def ringed(self, name, c, s):
        k = lax.rem(c, 2)
        return self.copies(name, c, [(self.rz.at[k, s - 1, h], self.rz.at[k, s, h], self.at(z=to)) for h, to in self.sides()])

    def d0(self, c):
        go(self.cr0(c))

    def d1(self, c):
        arrive(self.cr0(c))
        k = lax.rem(c, 2)
        for h in PAIR:
            own = self.dgrad(c, self.far(h, 3), part(h, HD))
            for j in FOUR:
                self.rz0[k, h, j] = b16(f32(self.rz0[k, h, j]) + f32(own[j]))
        go(self.cr1(c))
        leave(self.cr0(c))

    def d2(self, c):
        self.pass_on(c, self.cr1, self.cr2, 0)

    def d3(self, c):
        self.pass_on(c, self.cr2, self.cr3, 1)

    def pass_on(self, c, before, after, s):
        arrive(before(c))
        k = lax.rem(c, 2)
        for h in PAIR:
            own = self.dgrad(c, self.far(h, 2 - s))
            for j in FOUR:
                self.rz[k, s, h, j] = b16(f32(self.rz[k, s, h, j]) + f32(own[j]))
        go(after(c))
        leave(before(c))

    def cy(self, c):
        k = lax.rem(c, 2)
        ys = [self.up_y(i) for i in OTHERS]
        return self.copies("dy", c, [(self.sdy.at[y], self.rdy.at[k, i], self.at(y=y)) for i, y in enumerate(ys)])

    def dy_sum(self, c):
        arrive(self.cr3(c))
        k = lax.rem(c, 2)

        def total(j):
            return f32(self.rz[k, 2, 0, j]) + f32(self.rz[k, 2, 1, j]) + f32(self.dgrad(c, self.z)[j])

        for i in OTHERS:
            y = self.up_y(i)
            self.sdy[y] = b16(total(y))
        self.kdy[...] = total(self.y)
        go(self.cy(c))
        leave(self.cr3(c))

    def away(self, c):
        return self.up_x(-lax.rem(c, CHUNKS))

    def owner_sem(self, name, c):
        return FIRST[name] + lax.rem(c, 2) * COUNTS[name] - 1

    def to_owner(self, c, i, x):
        return self.copy(self.owner_sem("dx", c) + i, self.xb, self.fx.at[layer_of(c), i - 1], self.at(x=x))

    def dblock(self, c, y):
        return self.od.at[layer_of(c), lax.rem(c, CHUNKS), y, self.z]

    def from_owner(self, c, i, x):
        ref = self.dblock(c, self.y)
        return self.copy(self.owner_sem("ex", c) + i, ref, ref, self.at(x=x))

    def dx(self, c):
        arrive(self.cy(c))
        k = lax.rem(c, 2)
        v = self.kdy[...]
        for i in range(3):
            v = v + f32(self.rdy[k, i])
        self.xo[...] = v
        self.xb[...] = b16(v)

        @pl.when(self.away(c) > 0)
        def _():
            self.to_owner(c, self.away(c), lax.rem(c, CHUNKS)).start()

        leave(self.cy(c))

    def ex(self, c):
        l = layer_of(c)

        @pl.when(self.away(c) > 0)
        def _():
            self.to_owner(c, self.away(c), lax.rem(c, CHUNKS)).wait_send()

        @pl.when(self.away(c) == 0)
        def _():
            g = self.xo[...]
            for i in OTHERS:
                self.to_owner(c, i, self.up_x(i)).wait_recv()
                g = g + f32(self.fx[l, i - 1])
            self.dblock(c, self.y)[...], self.mod[l], self.vod[l] = adamw(f32(self.wd[l]), self.md[l], self.vd[l], f32(b16(g)))
            for i in OTHERS:
                self.from_owner(c, i, self.up_x(i)).start()

    def ey(self, c):
        @pl.when(self.away(c) > 0)
        def _():
            self.from_owner(c, self.away(c), lax.rem(c, CHUNKS)).wait_recv()

        @pl.when(self.away(c) == 0)
        def _():
            for i in OTHERS:
                self.from_owner(c, i, self.up_x(i)).wait_send()

        go(self.cz(c))

    def cz(self, c, get=False):
        out = []
        for i in OTHERS:
            y = self.up_y(-i if get else i)
            ref = self.dblock(c, y if get else self.y)
            out.append((ref, ref, self.at(y=y)))
        return self.copies("ey", c, out)

    def back(self, name, n, half=False):
        def moves(c, get=False):
            out = []
            for h, to in self.sides():
                ref = self.od.at[layer_of(c), lax.rem(c, CHUNKS), :, self.far(1 - h, n + get)]
                ref = ref.at[:, :, part(h, HD)] if half else ref
                out.append((ref, ref, self.at(z=to)))
            return self.copies(name, c, out)

        return moves

    def b0(self, c):
        arrive(self.cz(c, True))
        go(self.back("b0", 0)(c))
        leave(self.cz(c))

    def b1(self, c):
        self.hand_on(self.back("b0", 0), self.back("b1", 1), c)

    def b2(self, c):
        self.hand_on(self.back("b1", 1), self.back("b2", 2), c)

    def b3(self, c):
        self.hand_on(self.back("b2", 2), self.back("b3", 3, True), c)

    def dend(self, c):
        arrive(self.back("b3", 3, True)(c, True))
        leave(self.back("b3", 3, True)(c))


    def weights(self, i):
        l = jnp.where((i >= CHUNKS) & (i < LAST), 1, 0)
        k, ci = lax.rem(i, 2), lax.rem(i, CHUNKS)
        hidden = rows_of(ci, CW)
        pairs = ((self.w_gate.at[l, :, hidden], self.wcg), (self.w_up.at[l, :, hidden], self.wcu), (self.w_down.at[l, hidden], self.wcd))
        return [pltpu.make_async_copy(src, dst.at[k], self.wsem.at[k, i]) for i, (src, dst) in enumerate(pairs)]

    def scale(self, h):
        return lax.rsqrt(jnp.mean(h * h, -1, keepdims=True) + 1e-6)

    def sweep(self, body, n=SUB, lo=0, hi=None):
        def step(t, carry):
            body(rows_of(t, n))
            return carry

        lax.fori_loop(lo, TOK // n if hi is None else hi, step, 0)

    def turn(self, src, dst):
        for i in EIGHT:
            for j in PAIR:
                dst[part(j, SUB), part(i, SUB)] = b16(dot_t(self.eye[...], src[part(i, SUB), part(j, SUB)]))

    def normed(self, rows, h):
        h = f32(h)
        self.a[rows] = b16(h * self.scale(h))

    def start(self):
        i, j = (lax.broadcasted_iota(jnp.int32, (SUB, SUB), axis) for axis in PAIR)
        self.eye[...] = b16(jnp.where(i == j, 1.0, 0.0))
        self.acc[...] = jnp.zeros_like(self.acc)

    def start_rows(self):
        self.sweep(lambda rows: self.normed(rows, self.xv[rows]), BIG)

    def own_blocks(self):
        tiles = [(l, w, j) for l in PAIR for w in PAIR for j in FOUR]
        rows = rows_of(4 * self.x + self.y, 32)
        refs = (self.w_gate, self.w_up)
        out = [pltpu.make_async_copy(refs[w].at[l, rows, part(j, CW)], self.gb.at[l, w, j], self.osem.at[i]) for i, (l, w, j) in enumerate(tiles)]
        mine = rows_of(32 * self.x + 8 * self.y + self.z, 24)
        return out + [pltpu.make_async_copy(self.w_down.at[l, mine], self.wd.at[l], self.osem.at[len(tiles) + l]) for l in PAIR]

    def pick_rows(self):
        for l in PAIR:
            for j in FOUR:
                for w in PAIR:
                    v = f32(self.gb[l, w, j])
                    for z in EIGHT:
                        for h in PAIR:
                            self.zf[z, w, h] = v[4 * z : 4 * z + 4, h * HW : (h + 1) * HW]
                    for h in PAIR:
                        (self.wu if w else self.wg)[l, :, part(2 * j + h, HW)] = self.zf[self.z, w, h]

    def forward(self, i):
        k = lax.rem(i, 2)

        def tile(t, carry):
            rows = rows_of(t, BIG)

            @pl.when(i > 0)
            def _():
                self.save(i - 1, t).wait()

            a = self.a[rows]
            for n in range(CW // SUB):
                cols = part(n, SUB)
                g = dot(a, self.wcg[k, :, cols])
                u = dot(a, self.wcu[k, :, cols])
                s = 0.5 * jnp.tanh(0.5 * g) + 0.5
                self.act[rows, cols] = b16(g * s * u)
            self.acc[rows] += dot(self.act[rows], self.wcd[k])
            self.save(i, t).start()
            return carry

        lax.fori_loop(0, TOK // BIG, tile, 0)

    def layer_up(self):
        def body(rows):
            h = b16(f32(self.xv[rows]) + f32(b16(self.acc[rows])))
            self.h[rows] = h
            self.normed(rows, h)
            self.acc[rows] = jnp.zeros((BIG, D), F32)

        self.sweep(body, BIG)
        self.turn(self.a, self.at_)
        self.turn(self.dh, self.dht)

    def layer_down(self):
        def body(rows):
            h = f32(self.h[rows])
            s = self.scale(h)
            ct = f32(b16(self.acc[rows]))
            d = ct * s - h * (s * s * s * jnp.mean(ct * h, -1, keepdims=True))
            self.dh[rows] = b16(f32(self.dh[rows]) + f32(b16(d)))

        self.sweep(body, BIG)
        self.kept_a().wait()
        self.turn(self.a, self.at_)
        self.turn(self.dh, self.dht)

    def tiles(self, k, second, n, t):
        def body(rows):
            a, dh = self.a[rows], self.dh[rows]
            for i in range(CW // SUB):
                cols = part(i, SUB)
                g = dot(a, self.wcg[k, :, cols])
                u = dot(a, self.wcu[k, :, cols])
                d = f32(b16(dot_t(dh, self.wcd[k, cols])))
                s = 0.5 * jnp.tanh(0.5 * g) + 0.5
                sg = g * s
                if second:
                    self.act[rows, cols] = b16(sg * u)
                self.du[rows, cols] = b16(d * sg)
                self.dg[rows, cols] = b16(d * u * (s + sg * (1.0 - s)))
            if second:
                self.acc[rows] += dot_t(self.dg[rows], self.wcg[k]) + dot_t(self.du[rows], self.wcu[k])

        self.sweep(body, n, t, t + 1)

    def save(self, i, t):
        rows = rows_of(t, BIG)
        return pltpu.make_async_copy(self.act.at[rows], self.saved.at[i, rows], self.asem.at[t])

    def load(self, c):
        return pltpu.make_async_copy(self.saved.at[c - CHUNKS], self.act, self.asem.at[0])

    def keep_a(self):
        return pltpu.make_async_copy(self.a, self.saved_a, self.asem.at[2])

    def kept_a(self):
        return pltpu.make_async_copy(self.saved_a, self.a, self.asem.at[2])

    def grads_down(self, c):
        kd = lax.rem(c, 3)
        for n in range(CW // SUB):
            self.tmp[:, part(n, SUB)] = b16(dot(self.dht[...], self.act[:, part(n, SUB)]))
        for n in range(CW // SUB):
            v = dot_t(self.eye[...], self.tmp[:, part(n, SUB)])
            for i in range(SUB // 8):
                q, o = divmod(n * SUB + i * 8, 24)
                self.db[kd, q // 8, q % 8, o : o + 8, :] = b16(v[i * 8 : i * 8 + 8])

    def grads(self, k, w):
        src, dst = (self.du, self.ub) if w else (self.dg, self.gb)
        dst[k] = b16(dot(self.at_[...], src[...])).reshape(*GU, CW)


def vm(*shape, dtype=BF16):
    return pltpu.VMEM(shape, dtype)


GU = (4, 4, 32)
DN = (4, 8, 24, D)
SCRATCH = dict(
    h=vm(TOK, D), a=vm(TOK, D), at_=vm(D, TOK), dh=vm(TOK, D), dht=vm(D, TOK), acc=vm(TOK, D, dtype=F32),
    act=vm(TOK, CW), dg=vm(TOK, CW), du=vm(TOK, CW), eye=vm(SUB, SUB), tmp=vm(D, CW), wcg=vm(2, D, CW), wcu=vm(2, D, CW), wcd=vm(2, CW, D),
    gb=vm(2, *GU, CW), ub=vm(2, *GU, CW), db=vm(3, *DN),
    r1=vm(2, 2, 2, 2, 4, 32, HW), s2=vm(2, 2, 4, 32, HW), r2=vm(2, 2, 2, 4, 32, HW),
    s3=vm(2, 4, 2, 32, HW), r3=vm(2, 2, 3, 2, 32, HW), keep=vm(2, 2, 32, HW, dtype=F32),
    zf=vm(8, 2, 2, 4, HW, dtype=F32), zs=vm(8, 2, 2, 4, HW), zo=vm(2, 2, 4, HW, dtype=F32), fz=vm(7, 2, 2, 4, HW),
    nb=vm(2, 2, 4, HW), wz=vm(8, 2, 2, 4, HW), slab=vm(2, 32, CW, dtype=F32),
    rz0=vm(2, 2, 4, 24, HD), rz=vm(2, 3, 2, 4, 24, D), sdy=vm(4, 24, D), rdy=vm(2, 3, 24, D), kdy=vm(24, D, dtype=F32),
    xb=vm(24, D), xo=vm(24, D, dtype=F32), fx=vm(2, 3, 24, D), wg=vm(2, 4, FF, dtype=F32), wu=vm(2, 4, FF, dtype=F32), wd=vm(2, 24, D),
    ssem=pltpu.SemaphoreType.DMA((SEMS,)), rsem=pltpu.SemaphoreType.DMA((SEMS,)), osem=pltpu.SemaphoreType.DMA((18,)),
    wsem=pltpu.SemaphoreType.DMA((2, 3)), xsem=pltpu.SemaphoreType.DMA((2,)), asem=pltpu.SemaphoreType.DMA((3,)),
)
HBM_IN = ("x_in", "dy", "w_gate", "w_up", "w_down")
VMEM_IN = ("mg", "mu", "md", "vg", "vu", "vd")
OUT = ("og", "ou", "od", "mog", "mou", "mod", "vog", "vou", "vod", "saved", "saved_a")

SLOTS = 8
EVENTS = dict(
    w1=(7, 7),
    w2=(11, 11),
    wi=(14, 14),
    wf=(19, 19),
    renew=(23, 22),
    gi=(27, 27),
    g1=(32, 35),
    g2=(37, 42),
    gend=(40, 50),
    d0=(5, 0),
    d1=(7, 3),
    d2=(11, 7),
    d3=(14, 11),
    dy_sum=(18, 15),
    dx=(20, 18),
    ex=(22, 21),
    ey=(25, 24),
    b0=(30, 28),
    b1=(33, 34),
    b2=(41, 41),
    b3=(44, 46),
    dend=(52, 54),
)
SPAN = max(p for both in EVENTS.values() for p in both) // SLOTS


def kernel(*refs):
    names = HBM_IN + VMEM_IN + OUT + tuple(SCRATCH)
    q = Step(dict(zip(names, refs, strict=True)))
    q.xv = q.dg.at[:, part(0, D)]
    first = [pltpu.make_async_copy(src.at[0], dst, q.xsem.at[i]) for i, (src, dst) in enumerate(((q.x_in, q.xv), (q.dy, q.dh)))]
    go(first[:1] + q.weights(0))
    q.greet()
    run("start", q.start)
    first[0].wait()
    run("start_rows", q.start_rows)
    go(first[1:] + [q.keep_a()] + q.own_blocks())

    def forward(i, carry):
        go(q.weights(i + 1))
        for w in q.weights(i):
            w.wait()

        run("forward", q.forward, i)
        return carry

    lax.fori_loop(0, CHUNKS, forward, 0)
    first[1].wait()
    q.keep_a().wait()
    run("layer_up", q.layer_up)
    for t in PAIR:
        q.save(CHUNKS - 1, t).wait()
    for c in q.own_blocks():
        c.wait()
    run("pick_rows", q.pick_rows)
    run("greeted", q.greeted)

    def chunk(c, carry):
        k = lax.rem(c, 2)

        @pl.when(c < LAST - 1)
        def _():
            go(q.weights(c + CHUNKS + 1))

        @pl.when(c < LAST)
        def _():
            for w in q.weights(c + CHUNKS):
                w.wait()

        @pl.when(c == CHUNKS)
        def _():
            run("layer_down", q.layer_down)

        def down():
            q.load(c).wait()
            q.grads_down(c)

            @pl.when(c < LAST - 1)
            def _():
                q.load(c + 1).start()

        def down_second():
            q.grads_down(c)

            @pl.when(c == CHUNKS - 1)
            def _():
                q.load(c + 1).start()
                q.kept_a().start()

        second, first_, both = c < CHUNKS, (c >= CHUNKS) & (c < LAST), c < LAST
        pieces = {slot: [] for slot in range(SLOTS)}
        pieces[0].append((first_, down))
        for t in FOUR:
            pieces[1 + t].append((second, lambda t=t: q.tiles(k, True, T, t)))
        for t in PAIR:
            pieces[2 + 2 * t].append((first_, lambda t=t: q.tiles(k, False, BIG, t)))
            pieces[6 + t].append((both, lambda t=t: q.grads(k, t)))
        pieces[5].append((second, down_second))
        for slot in range(SLOTS):
            for when, piece in pieces[slot]:

                @pl.when(when)
                def _():
                    run("compute", piece)

            due = []
            for event, (second_at, first_at) in EVENTS.items():
                if second_at == first_at:
                    due.append((second_at, 0, LAST, event))
                else:
                    due += [(second_at, 0, CHUNKS, event), (first_at, CHUNKS, LAST, event)]
            for at, lo, hi, event in sorted(due, reverse=True):
                if at % SLOTS == slot:
                    back = at // SLOTS

                    @pl.when((c >= back + lo) & (c < back + hi))
                    def _():
                        run(event, getattr(q, event), c - back)

        return carry

    lax.fori_loop(0, LAST + SPAN, chunk, 0)


def run(name, f, *args):
    f(*args)


def place(*refs):
    n = len(refs) // 2
    copies = [pltpu.make_async_copy(src, dst, refs[-1].at[i]) for i, (src, dst) in enumerate(zip(refs[:n], refs[n:-1], strict=True))]
    go(copies)
    for c in copies:
        c.wait()


def solution(mesh):
    def local(x, dy, wg, wu, wd, *mv):
        hbm, vmem = (pl.BlockSpec(memory_space=s) for s in (pl.ANY, pltpu.VMEM))
        news = [jax.ShapeDtypeStruct((2, *s), BF16) for s in ((*GU, FF), (*GU, FF), (4, *DN))]
        moments = [jax.ShapeDtypeStruct(t.shape, F32) for t in mv]
        kept = [jax.ShapeDtypeStruct(s, BF16) for s in ((CHUNKS, TOK, CW), (TOK, D))]
        out = pl.pallas_call(
            kernel,
            name="step",
            out_shape=[pltpu.VMEM(t.shape, t.dtype) for t in news + moments] + kept,
            in_specs=[hbm] * 5 + [vmem] * 6,
            out_specs=[vmem] * 9 + [hbm] * 2,
            scratch_shapes=list(SCRATCH.values()),
            compiler_params=pltpu.CompilerParams(collective_id=1, has_side_effects=True, vmem_limit_bytes=VMEM_MAIN),
        )(x, dy, wg, wu, wd, *mv)
        placed = pl.pallas_call(
            place,
            name="place",
            out_shape=news + moments,
            in_specs=[vmem] * 9,
            out_specs=[hbm] * 9,
            scratch_shapes=[pltpu.SemaphoreType.DMA((9,))],
            compiler_params=pltpu.CompilerParams(vmem_limit_bytes=1 << 20),
        )(*out[:9])
        return *(t.reshape(w.shape) for t, w in zip(placed, (wg, wu, wd))), *placed[3:]

    rows, whole = P(None, "dp", None), P()
    return jax.shard_map(
        local,
        mesh=mesh,
        in_specs=(P(("rep", "dp"), None, None),) * 2 + (whole,) * 3 + (rows,) * 6,
        out_specs=(P("rep", None, None),) * 3 + (P("rep", "dp", None),) * 6,
        check_vma=False,
    )
```

```python
import jax
import jax.numpy as jnp
from jax import lax
from jax.experimental import pallas as pl
from jax.experimental.pallas import tpu as pltpu
from jax.sharding import PartitionSpec as P

MESH = pl.DeviceIdType.MESH
F32, BF16 = jnp.float32, jnp.bfloat16
TOK, D, FF = 2048, 512, 3072
CW = 768
HW = CW // 2
HF = FF // 2
HD = D // 2
LN = 128
CHUNKS = FF // CW
LAST = 2 * CHUNKS
PAIR = (0, 1)
FOUR = range(4)
EIGHT = range(8)
T = 512
BIG = 1024
SUB = 256
VMEM_MAIN = 47300000


def f32(v):
    return v.astype(F32)


def b16(v):
    return v.astype(BF16)


def dot(a, b):
    return jnp.dot(a, b, preferred_element_type=F32)


def dot_t(a, b):
    return lax.dot_general(a, b, (((1,), (1,)), ((), ())), preferred_element_type=F32)


def rows_of(t, n):
    return pl.ds(pl.multiple_of(t * n, n), n)


def part(i, n):
    return pl.ds(i * n, n)


def flip(p):
    return p + 1 - 2 * lax.rem(p, 2)


def mirror(p):
    return 3 - p


def partners(p, half):
    return (mirror(p), flip(p)) if half else (flip(p), mirror(p))


def passed(p, half):
    first, _ = partners(p, half)
    return first, partners(first, half)[1]


def kept(p, half):
    return p, partners(p, half)[1]


def layer_of(c):
    return jnp.where(c < CHUNKS, 1, 0)


def go(copies):
    for c in copies:
        c.start()


def arrive(copies):
    for c in copies:
        c.wait_recv()


def leave(copies):
    for c in copies:
        c.wait_send()


def adamw(w, m, v, g):
    m = 0.9 * m + 0.1 * g
    v = 0.95 * v + 0.05 * g * g
    step = m * lax.rsqrt(v + 1e-8) + 0.1 * w
    return b16(w - 0.02 * step), m, v


COUNTS = dict(c1=8, c2=4, c3=6, cf=7, a0=7, a1=6, a3=4, a4=8, r0=2, r1=4, r2=2, r3=2, dy=3, dx=3, ex=3, ey=3, b0=2, b1=2, b2=2, b3=2)
FIRST = {}
SEMS = 0
for _name, _n in COUNTS.items():
    FIRST[_name] = SEMS
    SEMS += 2 * _n
OTHERS = (1, 2, 3)


class Step:
    def __init__(self, refs):
        self.__dict__.update(refs)
        d = lax.axis_index("dp")
        self.rep = lax.axis_index("rep")
        self.x, self.y, self.z = d // 32, lax.rem(d // 8, 4), lax.rem(d, 8)


    def at(self, x=None, y=None, z=None):
        x = self.x if x is None else x
        y = self.y if y is None else y
        z = self.z if z is None else z
        return (self.rep, x * 32 + y * 8 + z)

    def up_z(self, i):
        return lax.rem(self.z + i + 16, 8)

    def up_x(self, i):
        return lax.rem(self.x + i + 4, 4)

    def up_y(self, i):
        return lax.rem(self.y + i + 4, 4)

    def up_inner(self, w, i):
        return self.up_x(i) if w else self.up_y(i)

    def copy(self, sem, src, dst, dev):
        return pltpu.make_async_remote_copy(
            src_ref=src, dst_ref=dst, send_sem=self.ssem.at[sem], recv_sem=self.rsem.at[sem], device_id=dev, device_id_type=MESH
        )

    def copies(self, name, c, moves):
        base = FIRST[name] + lax.rem(c, 2) * COUNTS[name]
        return [self.copy(base + i, *move) for i, move in enumerate(moves)]

    def peers(self):
        out = [self.at(z=self.up_z(i)) for i in range(1, 8)]
        return out + [self.at(x=self.up_x(i)) for i in OTHERS] + [self.at(y=self.up_y(i)) for i in OTHERS]

    def greet(self):
        b = pltpu.get_barrier_semaphore()
        for q in self.peers():
            pl.semaphore_signal(b, inc=1, device_id=q, device_id_type=MESH)

    def greeted(self):
        pl.semaphore_wait(pltpu.get_barrier_semaphore(), len(self.peers()))


    def outer(self, w):
        return self.y if w else self.x

    def inner(self, w):
        return self.x if w else self.y

    def at_outer(self, w, p):
        return self.at(y=p) if w else self.at(x=p)

    def at_inner(self, w, p):
        return self.at(x=p) if w else self.at(y=p)

    def halves(self):
        return [(w, h) for w in PAIR for h in PAIR]

    def block(self, w, k, b, h):
        cols = part(h, HW)
        return self.ub.at[k, :, b, :, cols] if w else self.gb.at[k, b, :, :, cols]

    def own(self, w, k, b, j, h):
        cols = part(h, HW)
        return f32(self.ub[k, j, b, :, cols] if w else self.gb[k, b, j, :, cols])

    def c1(self, c):
        k, out = lax.rem(c, 2), []
        for w, h in self.halves():
            first, _ = partners(self.outer(w), h)
            for i, b in enumerate(passed(self.outer(w), h)):
                out.append((self.block(w, k, b, h), self.r1.at[w, k, h, i], self.at_outer(w, first)))
        return self.copies("c1", c, out)

    def c2(self, c):
        k = lax.rem(c, 2)
        return self.copies("c2", c, [(self.s2.at[w, h], self.r2.at[w, k, h], self.at_outer(w, partners(self.outer(w), h)[1])) for w, h in self.halves()])

    def c3(self, c):
        k, out = lax.rem(c, 2), []
        for w in PAIR:
            for i in OTHERS:
                j = self.up_inner(w, i)
                out.append((self.s3.at[w, j], self.r3.at[w, k, i - 1], self.at_inner(w, j)))
        return self.copies("c3", c, out)

    def cf(self, c):
        zs = [self.up_z(i) for i in range(1, 8)]
        return self.copies("cf", c, [(self.zs.at[z], self.fz.at[i], self.at(z=z)) for i, z in enumerate(zs)])

    def w1(self, c):
        go(self.c1(c))

    def w2(self, c):
        arrive(self.c1(c))
        k = lax.rem(c, 2)
        for w, h in self.halves():
            _, b = partners(self.outer(w), h)
            for j in FOUR:
                self.s2[w, h, j] = b16(self.own(w, k, b, j, h) + f32(self.r1[w, k, h, 1, j]))
        go(self.c2(c))
        leave(self.c1(c))

    def wi(self, c):
        arrive(self.c2(c))
        k = lax.rem(c, 2)
        for w, h in self.halves():

            def total(j):
                return self.own(w, k, self.outer(w), j, h) + f32(self.r1[w, k, h, 0, j]) + f32(self.r2[w, k, h, j])

            for i in OTHERS:
                j = self.up_inner(w, i)
                self.s3[w, j, h] = b16(total(j))
            self.keep[w, h] = total(self.inner(w))
        go(self.c3(c))
        leave(self.c2(c))

    def wf(self, c):
        arrive(self.c3(c))
        k = lax.rem(c, 2)
        for w, h in self.halves():
            v = self.keep[w, h]
            for i in range(3):
                v = v + f32(self.r3[w, k, i, h])
            for z in EIGHT:
                self.zf[z, w, h] = v[4 * z : 4 * z + 4]
                self.zs[z, w, h] = b16(v[4 * z : 4 * z + 4])
        self.zo[...] = self.zf[self.z]
        go(self.cf(c))
        leave(self.c3(c))

    def renew(self, c):
        arrive(self.cf(c))
        l, ci = layer_of(c), lax.rem(c, CHUNKS)
        for w, h in self.halves():
            wb, m, v, mo, vo = (getattr(self, s + "gu"[w]) for s in ("w", "m", "v", "mo", "vo"))
            g = self.zo[w, h]
            for i in range(7):
                g = g + f32(self.fz[i, w, h])
            cols = rows_of(2 * ci + h, HW)
            new, mo[l, :, cols], vo[l, :, cols] = adamw(f32(wb[l, :, cols]), m[l, :, cols], v[l, :, cols], f32(b16(g)))
            self.nb[w, h] = new
            self.wz[self.z, w, h] = new
        go(self.a0(c))
        leave(self.cf(c))


    def a0(self, c, get=False):
        zs = [self.up_z(-i if get else i) for i in range(1, 8)]
        return self.copies("a0", c, [(self.nb, self.wz.at[z if get else self.z], self.at(z=z)) for z in zs])

    def cols(self, c, h):
        return rows_of(2 * lax.rem(c, CHUNKS) + h, HW)

    def obig(self, w, c, b, h):
        l, cols = layer_of(c), self.cols(c, h)
        return self.ou.at[l, :, b, :, cols] if w else self.og.at[l, b, :, :, cols]

    def orows(self, w, c, b):
        l, cols = layer_of(c), rows_of(lax.rem(c, CHUNKS), CW)
        return self.ou.at[l, b, self.y, :, cols] if w else self.og.at[l, self.x, b, :, cols]

    def a1(self, c, get=False):
        out = []
        for w in PAIR:
            for i in OTHERS:
                j = self.up_inner(w, -i if get else i)
                ref = self.orows(w, c, j if get else self.inner(w))
                out.append((ref, ref, self.at_inner(w, j)))
        return self.copies("a1", c, out)

    def a3(self, c, get=False):
        out = []
        for w, h in self.halves():
            _, q = partners(self.outer(w), h)
            ref = self.obig(w, c, q if get else self.outer(w), h)
            out.append((ref, ref, self.at_outer(w, q)))
        return self.copies("a3", c, out)

    def a4(self, c, get=False):
        out = []
        for w, h in self.halves():
            first, _ = partners(self.outer(w), h)
            refs = [self.obig(w, c, b, h) for b in (passed if get else kept)(self.outer(w), h)]
            out += [(ref, ref, self.at_outer(w, first)) for ref in refs]
        return self.copies("a4", c, out)

    def gi(self, c):
        arrive(self.a0(c, True))
        for w in PAIR:
            for h in PAIR:
                for z in EIGHT:
                    self.slab[w, 4 * z : 4 * z + 4, part(h, HW)] = f32(self.wz[z, w, h])
            self.orows(w, c, self.inner(w))[...] = b16(self.slab[w])
        go(self.a1(c))
        leave(self.a0(c))

    def g1(self, c):
        arrive(self.a1(c, True))
        go(self.a3(c))
        leave(self.a1(c))

    def g2(self, c):
        self.hand_on(self.a3, self.a4, c)

    def gend(self, c):
        arrive(self.a4(c, True))
        leave(self.a4(c))

    def hand_on(self, before, after, c):
        arrive(before(c, True))
        go(after(c))
        leave(before(c))


    def sides(self):
        return enumerate((self.up_z(1), self.up_z(-1)))

    def far(self, side, n):
        return self.up_z(-n if side else n)

    def dgrad(self, c, b, *cols):
        return self.db.at[(lax.rem(c, 3), slice(None), b, slice(None), *cols)]

    def cr0(self, c):
        k = lax.rem(c, 2)
        return self.copies("r0", c, [(self.dgrad(c, self.far(0, 4), part(h, HD)), self.rz0.at[k, h], self.at(z=to)) for h, to in self.sides()])

    def cr1(self, c):
        k, out = lax.rem(c, 2), []
        for h, to in self.sides():
            out.append((self.rz0.at[k, h], self.rz.at[k, 0, h, :, :, part(h, HD)], self.at(z=to)))
            out.append((self.dgrad(c, self.far(h, 3), part(1 - h, HD)), self.rz.at[k, 0, h, :, :, part(1 - h, HD)], self.at(z=to)))
        return self.copies("r1", c, out)

    def cr2(self, c):
        return self.ringed("r2", c, 1)

    def cr3(self, c):
        return self.ringed("r3", c, 2)

    def ringed(self, name, c, s):
        k = lax.rem(c, 2)
        return self.copies(name, c, [(self.rz.at[k, s - 1, h], self.rz.at[k, s, h], self.at(z=to)) for h, to in self.sides()])

    def d0(self, c):
        go(self.cr0(c))

    def d1(self, c):
        arrive(self.cr0(c))
        k = lax.rem(c, 2)
        for h in PAIR:
            own = self.dgrad(c, self.far(h, 3), part(h, HD))
            for j in FOUR:
                self.rz0[k, h, j] = b16(f32(self.rz0[k, h, j]) + f32(own[j]))
        go(self.cr1(c))
        leave(self.cr0(c))

    def d2(self, c):
        self.pass_on(c, self.cr1, self.cr2, 0)

    def d3(self, c):
        self.pass_on(c, self.cr2, self.cr3, 1)

    def pass_on(self, c, before, after, s):
        arrive(before(c))
        k = lax.rem(c, 2)
        for h in PAIR:
            own = self.dgrad(c, self.far(h, 2 - s))
            for j in FOUR:
                self.rz[k, s, h, j] = b16(f32(self.rz[k, s, h, j]) + f32(own[j]))
        go(after(c))
        leave(before(c))

    def cy(self, c):
        k = lax.rem(c, 2)
        ys = [self.up_y(i) for i in OTHERS]
        return self.copies("dy", c, [(self.sdy.at[y], self.rdy.at[k, i], self.at(y=y)) for i, y in enumerate(ys)])

    def dy_sum(self, c):
        arrive(self.cr3(c))
        k = lax.rem(c, 2)

        def total(j):
            return f32(self.rz[k, 2, 0, j]) + f32(self.rz[k, 2, 1, j]) + f32(self.dgrad(c, self.z)[j])

        for i in OTHERS:
            y = self.up_y(i)
            self.sdy[y] = b16(total(y))
        self.kdy[...] = total(self.y)
        go(self.cy(c))
        leave(self.cr3(c))

    def away(self, c):
        return self.up_x(-lax.rem(c, CHUNKS))

    def owner_sem(self, name, c):
        return FIRST[name] + lax.rem(c, 2) * COUNTS[name] - 1

    def to_owner(self, c, i, x):
        return self.copy(self.owner_sem("dx", c) + i, self.xb, self.fx.at[layer_of(c), i - 1], self.at(x=x))

    def dblock(self, c, y):
        return self.od.at[layer_of(c), lax.rem(c, CHUNKS), y, self.z]

    def from_owner(self, c, i, x):
        ref = self.dblock(c, self.y)
        return self.copy(self.owner_sem("ex", c) + i, ref, ref, self.at(x=x))

    def dx(self, c):
        arrive(self.cy(c))
        k = lax.rem(c, 2)
        v = self.kdy[...]
        for i in range(3):
            v = v + f32(self.rdy[k, i])
        self.xo[...] = v
        self.xb[...] = b16(v)

        @pl.when(self.away(c) > 0)
        def _():
            self.to_owner(c, self.away(c), lax.rem(c, CHUNKS)).start()

        leave(self.cy(c))

    def ex(self, c):
        l = layer_of(c)

        @pl.when(self.away(c) > 0)
        def _():
            self.to_owner(c, self.away(c), lax.rem(c, CHUNKS)).wait_send()

        @pl.when(self.away(c) == 0)
        def _():
            g = self.xo[...]
            for i in OTHERS:
                self.to_owner(c, i, self.up_x(i)).wait_recv()
                g = g + f32(self.fx[l, i - 1])
            self.dblock(c, self.y)[...], self.mod[l], self.vod[l] = adamw(f32(self.wd[l]), self.md[l], self.vd[l], f32(b16(g)))
            for i in OTHERS:
                self.from_owner(c, i, self.up_x(i)).start()

    def ey(self, c):
        @pl.when(self.away(c) > 0)
        def _():
            self.from_owner(c, self.away(c), lax.rem(c, CHUNKS)).wait_recv()

        @pl.when(self.away(c) == 0)
        def _():
            for i in OTHERS:
                self.from_owner(c, i, self.up_x(i)).wait_send()

        go(self.cz(c))

    def cz(self, c, get=False):
        out = []
        for i in OTHERS:
            y = self.up_y(-i if get else i)
            ref = self.dblock(c, y if get else self.y)
            out.append((ref, ref, self.at(y=y)))
        return self.copies("ey", c, out)

    def back(self, name, n, half=False):
        def moves(c, get=False):
            out = []
            for h, to in self.sides():
                ref = self.od.at[layer_of(c), lax.rem(c, CHUNKS), :, self.far(1 - h, n + get)]
                ref = ref.at[:, :, part(h, HD)] if half else ref
                out.append((ref, ref, self.at(z=to)))
            return self.copies(name, c, out)

        return moves

    def b0(self, c):
        arrive(self.cz(c, True))
        go(self.back("b0", 0)(c))
        leave(self.cz(c))

    def b1(self, c):
        self.hand_on(self.back("b0", 0), self.back("b1", 1), c)

    def b2(self, c):
        self.hand_on(self.back("b1", 1), self.back("b2", 2), c)

    def b3(self, c):
        self.hand_on(self.back("b2", 2), self.back("b3", 3, True), c)

    def dend(self, c):
        arrive(self.back("b3", 3, True)(c, True))
        leave(self.back("b3", 3, True)(c))


    def weights(self, i):
        l = jnp.where((i >= CHUNKS) & (i < LAST), 1, 0)
        k, ci = lax.rem(i, 2), lax.rem(i, CHUNKS)
        hidden = rows_of(ci, CW)
        pairs = ((self.w_gate.at[l, :, hidden], self.wcg), (self.w_up.at[l, :, hidden], self.wcu), (self.w_down.at[l, hidden], self.wcd))
        return [pltpu.make_async_copy(src, dst.at[k], self.wsem.at[k, i]) for i, (src, dst) in enumerate(pairs)]

    def scale(self, h):
        return lax.rsqrt(jnp.mean(h * h, -1, keepdims=True) + 1e-6)

    def sweep(self, body, n=SUB, lo=0, hi=None):
        def step(t, carry):
            body(rows_of(t, n))
            return carry

        lax.fori_loop(lo, TOK // n if hi is None else hi, step, 0)

    def turn(self, src, dst):
        for i in EIGHT:
            for j in PAIR:
                dst[part(j, SUB), part(i, SUB)] = b16(dot_t(self.eye[...], src[part(i, SUB), part(j, SUB)]))

    def normed(self, rows, h):
        h = f32(h)
        self.a[rows] = b16(h * self.scale(h))

    def start(self):
        i, j = (lax.broadcasted_iota(jnp.int32, (SUB, SUB), axis) for axis in PAIR)
        self.eye[...] = b16(jnp.where(i == j, 1.0, 0.0))
        self.acc[...] = jnp.zeros_like(self.acc)

    def start_rows(self):
        self.sweep(lambda rows: self.normed(rows, self.xv[rows]), BIG)

    def own_blocks(self):
        tiles = [(l, w, j) for l in PAIR for w in PAIR for j in FOUR]
        rows = rows_of(4 * self.x + self.y, 32)
        refs = (self.w_gate, self.w_up)
        out = [pltpu.make_async_copy(refs[w].at[l, rows, part(j, CW)], self.gb.at[l, w, j], self.osem.at[i]) for i, (l, w, j) in enumerate(tiles)]
        mine = rows_of(32 * self.x + 8 * self.y + self.z, 24)
        return out + [pltpu.make_async_copy(self.w_down.at[l, mine], self.wd.at[l], self.osem.at[len(tiles) + l]) for l in PAIR]

    def pick_rows(self):
        for l in PAIR:
            for j in FOUR:
                for w in PAIR:
                    v = f32(self.gb[l, w, j])
                    for z in EIGHT:
                        for h in PAIR:
                            self.zf[z, w, h] = v[4 * z : 4 * z + 4, h * HW : (h + 1) * HW]
                    for h in PAIR:
                        (self.wu if w else self.wg)[l, :, part(2 * j + h, HW)] = self.zf[self.z, w, h]

    def forward(self, i):
        k = lax.rem(i, 2)

        def tile(t, carry):
            rows = rows_of(t, BIG)

            @pl.when(i > 0)
            def _():
                self.save(i - 1, t).wait()

            a = self.a[rows]
            for n in range(CW // SUB):
                cols = part(n, SUB)
                g = dot(a, self.wcg[k, :, cols])
                u = dot(a, self.wcu[k, :, cols])
                s = 0.5 * jnp.tanh(0.5 * g) + 0.5
                self.act[rows, cols] = b16(g * s * u)
            self.acc[rows] += dot(self.act[rows], self.wcd[k])
            self.save(i, t).start()
            return carry

        lax.fori_loop(0, TOK // BIG, tile, 0)

    def layer_up(self):
        def body(rows):
            h = b16(f32(self.xv[rows]) + f32(b16(self.acc[rows])))
            self.h[rows] = h
            self.normed(rows, h)
            self.acc[rows] = jnp.zeros((BIG, D), F32)

        self.sweep(body, BIG)
        self.turn(self.a, self.at_)
        self.turn(self.dh, self.dht)

    def layer_down(self):
        def body(rows):
            h = f32(self.h[rows])
            s = self.scale(h)
            ct = f32(b16(self.acc[rows]))
            d = ct * s - h * (s * s * s * jnp.mean(ct * h, -1, keepdims=True))
            self.dh[rows] = b16(f32(self.dh[rows]) + f32(b16(d)))

        self.sweep(body, BIG)
        self.kept_a().wait()
        self.turn(self.a, self.at_)
        self.turn(self.dh, self.dht)

    def tiles(self, k, second, n, t):
        def body(rows):
            a, dh = self.a[rows], self.dh[rows]
            for i in range(CW // SUB):
                cols = part(i, SUB)
                g = dot(a, self.wcg[k, :, cols])
                u = dot(a, self.wcu[k, :, cols])
                d = f32(b16(dot_t(dh, self.wcd[k, cols])))
                s = 0.5 * jnp.tanh(0.5 * g) + 0.5
                sg = g * s
                if second:
                    self.act[rows, cols] = b16(sg * u)
                self.du[rows, cols] = b16(d * sg)
                self.dg[rows, cols] = b16(d * u * (s + sg * (1.0 - s)))
            if second:
                self.acc[rows] += dot_t(self.dg[rows], self.wcg[k]) + dot_t(self.du[rows], self.wcu[k])

        self.sweep(body, n, t, t + 1)

    def save(self, i, t):
        rows = rows_of(t, BIG)
        return pltpu.make_async_copy(self.act.at[rows], self.saved.at[i, rows], self.asem.at[t])

    def load(self, c):
        return pltpu.make_async_copy(self.saved.at[c - CHUNKS], self.act, self.asem.at[0])

    def keep_a(self):
        return pltpu.make_async_copy(self.a, self.saved_a, self.asem.at[2])

    def kept_a(self):
        return pltpu.make_async_copy(self.saved_a, self.a, self.asem.at[2])

    def grads_down(self, c):
        kd = lax.rem(c, 3)
        for n in range(CW // SUB):
            self.tmp[:, part(n, SUB)] = b16(dot(self.dht[...], self.act[:, part(n, SUB)]))
        for n in range(CW // SUB):
            v = dot_t(self.eye[...], self.tmp[:, part(n, SUB)])
            for i in range(SUB // 8):
                q, o = divmod(n * SUB + i * 8, 24)
                self.db[kd, q // 8, q % 8, o : o + 8, :] = b16(v[i * 8 : i * 8 + 8])

    def grads(self, k, w):
        src, dst = (self.du, self.ub) if w else (self.dg, self.gb)
        dst[k] = b16(dot(self.at_[...], src[...])).reshape(*GU, CW)


def vm(*shape, dtype=BF16):
    return pltpu.VMEM(shape, dtype)


GU = (4, 4, 32)
DN = (4, 8, 24, D)
SCRATCH = dict(
    h=vm(TOK, D), a=vm(TOK, D), at_=vm(D, TOK), dh=vm(TOK, D), dht=vm(D, TOK), acc=vm(TOK, D, dtype=F32),
    act=vm(TOK, CW), dg=vm(TOK, CW), du=vm(TOK, CW), eye=vm(SUB, SUB), tmp=vm(D, CW), wcg=vm(2, D, CW), wcu=vm(2, D, CW), wcd=vm(2, CW, D),
    gb=vm(2, *GU, CW), ub=vm(2, *GU, CW), db=vm(3, *DN),
    r1=vm(2, 2, 2, 2, 4, 32, HW), s2=vm(2, 2, 4, 32, HW), r2=vm(2, 2, 2, 4, 32, HW),
    s3=vm(2, 4, 2, 32, HW), r3=vm(2, 2, 3, 2, 32, HW), keep=vm(2, 2, 32, HW, dtype=F32),
    zf=vm(8, 2, 2, 4, HW, dtype=F32), zs=vm(8, 2, 2, 4, HW), zo=vm(2, 2, 4, HW, dtype=F32), fz=vm(7, 2, 2, 4, HW),
    nb=vm(2, 2, 4, HW), wz=vm(8, 2, 2, 4, HW), slab=vm(2, 32, CW, dtype=F32),
    rz0=vm(2, 2, 4, 24, HD), rz=vm(2, 3, 2, 4, 24, D), sdy=vm(4, 24, D), rdy=vm(2, 3, 24, D), kdy=vm(24, D, dtype=F32),
    xb=vm(24, D), xo=vm(24, D, dtype=F32), fx=vm(2, 3, 24, D), wg=vm(2, 4, FF, dtype=F32), wu=vm(2, 4, FF, dtype=F32), wd=vm(2, 24, D),
    ssem=pltpu.SemaphoreType.DMA((SEMS,)), rsem=pltpu.SemaphoreType.DMA((SEMS,)), osem=pltpu.SemaphoreType.DMA((18,)),
    wsem=pltpu.SemaphoreType.DMA((2, 3)), xsem=pltpu.SemaphoreType.DMA((2,)), asem=pltpu.SemaphoreType.DMA((3,)),
)
HBM_IN = ("x_in", "dy", "w_gate", "w_up", "w_down")
VMEM_IN = ("mg", "mu", "md", "vg", "vu", "vd")
OUT = ("og", "ou", "od", "mog", "mou", "mod", "vog", "vou", "vod", "saved", "saved_a")

SLOTS = 8
EVENTS = dict(
    w1=(7, 7),
    w2=(11, 11),
    wi=(14, 14),
    wf=(19, 19),
    renew=(23, 22),
    gi=(27, 27),
    g1=(32, 35),
    g2=(37, 42),
    gend=(43, 46),
    d0=(5, 0),
    d1=(7, 3),
    d2=(11, 7),
    d3=(14, 11),
    dy_sum=(18, 15),
    dx=(20, 18),
    ex=(22, 20),
    ey=(25, 24),
    b0=(30, 28),
    b1=(33, 34),
    b2=(41, 41),
    b3=(44, 45),
    dend=(49, 53),
)
SPAN = max(p for both in EVENTS.values() for p in both) // SLOTS


def kernel(*refs):
    names = HBM_IN + VMEM_IN + OUT + tuple(SCRATCH)
    q = Step(dict(zip(names, refs, strict=True)))
    q.xv = q.dg.at[:, part(0, D)]
    first = [pltpu.make_async_copy(src.at[0], dst, q.xsem.at[i]) for i, (src, dst) in enumerate(((q.x_in, q.xv), (q.dy, q.dh)))]
    go(first[:1] + q.weights(0))
    q.greet()
    run("start", q.start)
    first[0].wait()
    run("start_rows", q.start_rows)
    go(first[1:] + [q.keep_a()] + q.own_blocks())

    def forward(i, carry):
        go(q.weights(i + 1))
        for w in q.weights(i):
            w.wait()

        run("forward", q.forward, i)
        return carry

    lax.fori_loop(0, CHUNKS, forward, 0)
    first[1].wait()
    q.keep_a().wait()
    run("layer_up", q.layer_up)
    for t in PAIR:
        q.save(CHUNKS - 1, t).wait()
    for c in q.own_blocks():
        c.wait()
    run("pick_rows", q.pick_rows)
    run("greeted", q.greeted)

    def chunk(c, carry):
        k = lax.rem(c, 2)

        @pl.when(c < LAST - 1)
        def _():
            go(q.weights(c + CHUNKS + 1))

        @pl.when(c < LAST)
        def _():
            for w in q.weights(c + CHUNKS):
                w.wait()

        @pl.when(c == CHUNKS)
        def _():
            run("layer_down", q.layer_down)

        def down():
            q.load(c).wait()
            q.grads_down(c)

            @pl.when(c < LAST - 1)
            def _():
                q.load(c + 1).start()

        def down_second():
            q.grads_down(c)

            @pl.when(c == CHUNKS - 1)
            def _():
                q.load(c + 1).start()
                q.kept_a().start()

        second, first_, both = c < CHUNKS, (c >= CHUNKS) & (c < LAST), c < LAST
        pieces = {slot: [] for slot in range(SLOTS)}
        pieces[0].append((first_, down))
        for t in FOUR:
            pieces[1 + t].append((second, lambda t=t: q.tiles(k, True, T, t)))
        for t in PAIR:
            pieces[2 + 2 * t].append((first_, lambda t=t: q.tiles(k, False, BIG, t)))
            pieces[6 + t].append((both, lambda t=t: q.grads(k, t)))
        pieces[5].append((second, down_second))
        for slot in range(SLOTS):
            for when, piece in pieces[slot]:

                @pl.when(when)
                def _():
                    run("compute", piece)

            due = []
            for event, (second_at, first_at) in EVENTS.items():
                if second_at == first_at:
                    due.append((second_at, 0, LAST, event))
                else:
                    due += [(second_at, 0, CHUNKS, event), (first_at, CHUNKS, LAST, event)]
            for at, lo, hi, event in sorted(due, reverse=True):
                if at % SLOTS == slot:
                    back = at // SLOTS

                    @pl.when((c >= back + lo) & (c < back + hi))
                    def _():
                        run(event, getattr(q, event), c - back)

        return carry

    lax.fori_loop(0, LAST + SPAN, chunk, 0)


def run(name, f, *args):
    f(*args)


def place(*refs):
    n = len(refs) // 2
    pairs = list(zip(refs[:n], refs[n:-1], strict=True))
    copies = [pltpu.make_async_copy(src.at[l], dst.at[l], refs[-1].at[i, l]) for i, (src, dst) in enumerate(pairs) for l in PAIR]
    go(copies)
    for c in copies:
        c.wait()


def solution(mesh):
    def local(x, dy, wg, wu, wd, *mv):
        hbm, vmem = (pl.BlockSpec(memory_space=s) for s in (pl.ANY, pltpu.VMEM))
        news = [jax.ShapeDtypeStruct((2, *s), BF16) for s in ((*GU, FF), (*GU, FF), (4, *DN))]
        moments = [jax.ShapeDtypeStruct(t.shape, F32) for t in mv]
        kept = [jax.ShapeDtypeStruct(s, BF16) for s in ((CHUNKS, TOK, CW), (TOK, D))]
        out = pl.pallas_call(
            kernel,
            name="step",
            out_shape=[pltpu.VMEM(t.shape, t.dtype) for t in news + moments] + kept,
            in_specs=[hbm] * 5 + [vmem] * 6,
            out_specs=[vmem] * 9 + [hbm] * 2,
            scratch_shapes=list(SCRATCH.values()),
            compiler_params=pltpu.CompilerParams(collective_id=1, has_side_effects=True, vmem_limit_bytes=VMEM_MAIN),
        )(x, dy, wg, wu, wd, *mv)
        placed = pl.pallas_call(
            place,
            name="place",
            out_shape=news + moments,
            in_specs=[vmem] * 9,
            out_specs=[hbm] * 9,
            scratch_shapes=[pltpu.SemaphoreType.DMA((9, 2))],
            compiler_params=pltpu.CompilerParams(vmem_limit_bytes=1 << 20),
        )(*out[:9])
        return *(t.reshape(w.shape) for t, w in zip(placed, (wg, wu, wd))), *placed[3:]

    rows, whole = P(None, "dp", None), P()
    return jax.shard_map(
        local,
        mesh=mesh,
        in_specs=(P(("rep", "dp"), None, None),) * 2 + (whole,) * 3 + (rows,) * 6,
        out_specs=(P("rep", None, None),) * 3 + (P("rep", "dp", None),) * 6,
        check_vma=False,
    )
```
